256 devices in a mesh: section: 4 (over y), space: 64 (over z, x, core).
Axes of the slice: x: 4, y: 4, z: 8, core: 2. Of those that a mesh axis runs over, the one named last changes fastest.
Arguments:
- start_state: float32 [8, 6, 512, 512], P(None, None, 'space'), may hold values from -6 to 6
- stiffness: float32 [2, 512, 512], P(None, 'space'), may hold values from 0.5 to 4
- contact_a: int32 [8, 64, 8], P('section', 'space'), may hold values from 0 to 31
- contact_b: int32 [8, 64, 8], P('section', 'space'), may hold values from 0 to 39
- pair_count: int32 [8, 64], P('section', 'space'), may hold values from 1 to 8, 260 in all within a row
- cotangent: float32 [8, 6, 512, 512], P(None, None, 'space'), may hold values from -6 to 6
Outputs:
- exit_state: float32 [4, 8, 6, 512, 512], P('section', None, None, 'space')
- incoming_state_gradient: float32 [4, 8, 6, 512, 512], P('section', None, None, 'space')
- stiffness_grad: float32 [2, 512, 512], P(None, 'space')
The draws below stay inside these ranges and needn't reach their ends.
Inputs may be any that keep to these rules, and one draw needn't show every extreme that they name: Tiles are numbered within one device's band: contact_a over its own 8 rows, contact_b over those rows with one row added above and below, the upper added row first. Slots at or beyond pair_count are ignored; at every step some device has all 8 slots live.
All inputs are finite; a program needn't handle non-finite values.
Results may differ from the reference program's by a relative error of at most 0.0003.
Values sent between devices are 32-bit elements; how exact they have to be, the bound alone decides.
No kernel may reach another device: no remote copies, remote signals or barrier semaphores. Data moves between devices by JAX's collectives and lax.ppermute only.
A program may use at most 64 MiB of HBM per device.

```python
import math
import jax
import jax.numpy as jnp
import numpy as np
from jax import lax

COLS = 512
MICRO = 8
SECTION_STEPS = 2
PAIRS = 8
ROWS = 512
STEPS = 8
TILES_DEV = 32
N_SECTION = 4
N_SPACE = 64


def set_ends(result, key, low, largest):
    longest = result.shape.index(max(result.shape))
    spots = []
    for shift in (0, 1):
        where = [jax.random.randint(jax.random.fold_in(key, axis), (), 0, length) for axis, length in enumerate(result.shape)]
        where[longest] = (where[longest] + shift) % result.shape[longest]
        spots.append(tuple(where))
    return result.at[spots[0]].set(low).at[spots[1]].set(largest)


def level_of(rng, extent, cuts, smallest, largest):
    loudness, own = 1.0, jax.random.fold_in(rng, 6)
    for dim, parts in cuts:
        steps = jnp.exp(jax.random.uniform(jax.random.fold_in(own, dim), (parts,), jnp.float32, smallest / len(cuts), largest / len(cuts)))
        loudness = loudness * jnp.repeat(steps, extent[dim] // parts).reshape([-1 if axis == dim else 1 for axis in range(len(extent))])
    return loudness


def profile(number_of, total, limit, lean):
    portions = [(1 << 20) // math.isqrt(standing ** lean) + 1 for standing in range(2, number_of + 1)]
    spare, holding = total - limit - (number_of - 1), [1] * (number_of - 1)
    while spare > 0:
        movable = [i for i in range(number_of - 1) if holding[i] < limit]
        mass, budget = sum([portions[i] for i in movable]), spare
        for i in movable:
            extra = min(limit - holding[i], max(1, budget * portions[i] // mass), spare)
            holding[i] = holding[i] + extra
            spare = spare - extra
    return np.array([limit] + holding)


def ragged(rng, amount, total, most, skew):
    if amount == 2:
        one = jax.random.randint(rng, (), max(1, total - most), min(most, total - 1) + 1)
        return jnp.stack([one, total - one])
    sizes = jnp.asarray(profile(amount, total, most, skew), jnp.int32)
    pairs = (amount - 1) // 2
    giver, sink = sizes[1:1 + 2 * pairs:2], sizes[2:2 + 2 * pairs:2]
    room = jnp.minimum(giver - 1, most - sink)
    shifted = jax.random.randint(jax.random.fold_in(rng, 1), (pairs,), 0, 1 << 20) % (room + 1)
    sizes = sizes.at[1:1 + 2 * pairs:2].set(giver - shifted).at[2:2 + 2 * pairs:2].set(sink + shifted)
    return sizes[jax.random.permutation(jax.random.fold_in(rng, 2), amount)]


def scatter_about(stream_key, dims, width, reach, shards=(), held_as=jnp.bfloat16):
    array = width * jax.random.normal(stream_key, dims, jnp.float32)
    if shards:
        array = array * level_of(stream_key, dims, shards, -0.22, 0.18)
    return jnp.clip(array, -reach, reach).astype(held_as)


def setup_inputs(seed: int = 0) -> dict:
    key_of = jax.random.split(jax.random.key(seed), 7)
    return {
        "start_state": scatter_about(key_of[0], (MICRO, 6, ROWS, COLS), 1.0, 6.0, ((2, 64),), jnp.float32),
        "stiffness": jnp.clip(jnp.exp(math.log(4.0) - 2.0794415 * jax.random.uniform(key_of[1], (2, ROWS, COLS), jnp.float32) ** level_of(key_of[1], (2, ROWS, COLS), ((1, 64),), -0.2, 0.2)), 0.5, 4.0),
        "contact_a": set_ends(jax.random.randint(key_of[2], (STEPS, N_SPACE, PAIRS), 0, TILES_DEV), jax.random.fold_in(key_of[2], 1), 0, TILES_DEV - 1).astype(jnp.int32),
        "contact_b": set_ends(jax.random.randint(key_of[3], (STEPS, N_SPACE, PAIRS), 0, TILES_DEV + 2 * COLS // 128), jax.random.fold_in(key_of[3], 1), 0, (TILES_DEV + 2 * COLS // 128) - 1).astype(jnp.int32),
        "pair_count": jax.vmap(lambda own: ragged(own, N_SPACE, (N_SPACE + 1) * PAIRS // 2, PAIRS, 2))(jax.random.split(key_of[4], STEPS)).reshape((STEPS, N_SPACE)).astype(jnp.int32),
        "cotangent": scatter_about(key_of[5], (MICRO, 6, ROWS, COLS), 1.0, 6.0, ((2, 64),), jnp.float32),
    }


time_step = 0.1
damping = 0.98
rest_length = 1.0
contact_scale = 0.3
kernel_spread = 2.0
gravity = 0.5
tiny_length = 1e-06

def spring(offset, edge_constant):
    length = jnp.sqrt(lax.optimization_barrier(jnp.sum(offset * offset, axis=0)) + tiny_length)
    return (edge_constant * (length - rest_length) / length)[None] * offset

def contact(points, extended, hits_a, hits_b, active):
    tiles_own = points.reshape(3, -1, 128)
    tiles_all = extended.reshape(3, -1, 128)
    own_points = jnp.einsum('pt,ctk->cpk', hits_a, tiles_own, precision=lax.Precision.HIGHEST)
    other_points = jnp.einsum('pt,ctk->cpk', hits_b, tiles_all, precision=lax.Precision.HIGHEST)
    separation = own_points[:, :, :, None] - other_points[:, :, None, :]
    spring_weights = jnp.exp(-lax.optimization_barrier(jnp.sum(separation * separation, axis=0)) / kernel_spread) * active[:, None, None]
    repulsion = 2.0 * contact_scale / kernel_spread * lax.optimization_barrier(jnp.sum(spring_weights[None] * separation, axis=3))
    placed = jnp.einsum('pt,cpk->ctk', hits_a, repulsion, precision=lax.Precision.HIGHEST)
    return placed.reshape(points.shape)

def local_step(extended, velocity, stiff_row, stiff_column, hits_a, hits_b, active):
    points = extended[:, 1:-1]
    row_width = points.shape[2]
    column_mask = (lax.broadcasted_iota(jnp.int32, (1, row_width), 1) < row_width - 1).astype(stiff_row.dtype)
    right_edge = stiff_row * column_mask
    left_edge = jnp.pad(right_edge[:, :-1], ((0, 0), (1, 0)))
    right_points = jnp.pad(points[:, :, 1:], ((0, 0), (0, 0), (0, 1)))
    left_points = jnp.pad(points[:, :, :-1], ((0, 0), (0, 0), (1, 0)))
    total_force = spring(right_points - points, right_edge) + spring(left_points - points, left_edge)
    total_force = total_force + spring(extended[:, :-2] - points, stiff_column[:-1])
    total_force = total_force + spring(extended[:, 2:] - points, stiff_column[1:])
    total_force = total_force + contact(points, extended, hits_a, hits_b, active)
    gravity_pull = jnp.zeros((3, 1, 1), total_force.dtype).at[2].set(-gravity)
    velocity_new = damping * (velocity + time_step * (total_force + gravity_pull))
    points_new = points + time_step * velocity_new
    return jnp.concatenate([points_new, velocity_new], axis=0)

def tables(first_tiles, second_tiles, live_count, tiles_own, tiles_all, float_type):
    slot_count = first_tiles.shape[0]
    hits_a = (first_tiles[:, None] == lax.broadcasted_iota(jnp.int32, (slot_count, tiles_own), 1)).astype(float_type)
    hits_b = (second_tiles[:, None] == lax.broadcasted_iota(jnp.int32, (slot_count, tiles_all), 1)).astype(float_type)
    active = (lax.iota(jnp.int32, slot_count) < live_count).astype(float_type)
    return (hits_a, hits_b, active)

def region_step(state_now, stiff_row, stiff_masked, first_tiles, second_tiles, live_count):
    spaces = first_tiles.shape[0]
    total_rows = state_now.shape[1]
    row_width = state_now.shape[2]
    own_rows = total_rows // spaces
    padded = jnp.pad(state_now[:3], ((0, 0), (1, 1), (0, 0)))
    column_all = jnp.concatenate([jnp.zeros((1, row_width), stiff_masked.dtype), stiff_masked], axis=0)
    checked_step = jax.checkpoint(local_step)

    def region_one(space_index):
        start_row = space_index * own_rows
        extended = lax.dynamic_slice_in_dim(padded, start_row, own_rows + 2, 1)
        velocity = lax.dynamic_slice_in_dim(state_now[3:], start_row, own_rows, 1)
        own_row = lax.dynamic_slice_in_dim(stiff_row, start_row, own_rows, 0)
        own_column = lax.dynamic_slice_in_dim(column_all, start_row, own_rows + 1, 0)
        hits_a, hits_b, active = tables(first_tiles[space_index], second_tiles[space_index], live_count[space_index], own_rows * row_width // 128, (own_rows + 2) * row_width // 128, state_now.dtype)
        return checked_step(extended, velocity, own_row, own_column, hits_a, hits_b, active)
    blocks = lax.map(region_one, jnp.arange(spaces, dtype=jnp.int32))
    return blocks.transpose(1, 0, 2, 3).reshape(6, total_rows, row_width)

def reference(start_state, stiffness, contact_a, contact_b, pair_count, cotangent):
    total_rows = stiffness.shape[1]
    row_mask = (jnp.arange(total_rows, dtype=jnp.int32) < total_rows - 1).astype(stiffness.dtype)[:, None]

    def advance(state_now, stiff_row, stiff_column, section_total):
        masked = stiff_column * row_mask
        return jax.vmap(region_step, in_axes=(0, None, None, None, None, None))(state_now, stiff_row, masked, contact_a[section_total], contact_b[section_total], pair_count[section_total])
    visited = []
    leaving_state_list = []
    state_now = start_state
    for section_ordinal in range(N_SECTION):
        for section_inner_step in range(SECTION_STEPS):
            section_total = section_ordinal * SECTION_STEPS + section_inner_step
            visited.append(state_now)
            state_now = advance(state_now, stiffness[0], stiffness[1], section_total)
        leaving_state_list.append(state_now)
    adjoint = cotangent
    grad_row = jnp.zeros_like(stiffness[0])
    grad_column = jnp.zeros_like(stiffness[1])
    adjoint_list = [None] * N_SECTION
    for section_ordinal in reversed(range(N_SECTION)):
        for section_inner_step in reversed(range(SECTION_STEPS)):
            section_total = section_ordinal * SECTION_STEPS + section_inner_step

            def forward_one(state_in, row_in, column_in, section_total=section_total):
                return advance(state_in, row_in, column_in, section_total)
            _, pullback = jax.vjp(forward_one, visited[section_total], stiffness[0], stiffness[1])
            adjoint, part_row, part_column = pullback(adjoint)
            grad_row = grad_row + part_row
            grad_column = grad_column + part_column
        adjoint_list[section_ordinal] = adjoint
    return (jnp.stack(leaving_state_list), jnp.stack(adjoint_list), jnp.stack([grad_row, grad_column]))
```

```python
import functools

import jax
import jax.numpy as jnp
from jax import lax
from jax.experimental import pallas as pl
from jax.experimental.pallas import tpu as pltpu
from jax.sharding import PartitionSpec as P


H = 0.1
DAMP = 0.98
SCALE = 0.3
GRAV = 0.5
TINY = 1e-06
F32 = jnp.float32
BF16 = jnp.bfloat16
GROUP = 2
SLOTS = 8
ROWS = 8
COLS = 512
NB = COLS // 128
EXT = ROWS + 2
META_S, META_C, META_Q = 24, 25, 26


def lists(meta, step):
    section = meta[0, META_S]
    row = lax.rem(section - step // 2 + 4, 4)
    base = 32 * (step % 2)
    return row, base


def tile_start(row, block):
    return pl.multiple_of((block * EXT + row) * 8, 8)


def row_is(r, n=COLS):
    return lax.broadcasted_iota(jnp.int32, (ROWS, n), 0) == r


def fill_tiles(tiles, value_of):
    for t in range(2):
        for c in range(3):
            v = value_of(t, c)
            for b in range(NB):
                tiles[pl.ds((b * EXT + 1) * 8 + 3 * t + c, ROWS, stride=8), :] = v[:, b * 128 : (b + 1) * 128]


def read_tiles(tiles, k):
    return jnp.concatenate([tiles[pl.ds((b * EXT + 1) * 8 + k, ROWS, stride=8), :] for b in range(NB)], axis=1)


def fill_halo(tiles, up, down):
    for b in range(NB):
        tiles[pl.ds(b * EXT * 8, 8), :] = up[:, b * 128 : (b + 1) * 128]
        tiles[pl.ds((b * EXT + EXT - 1) * 8, 8), :] = down[:, b * 128 : (b + 1) * 128]


def selectors():
    row = lax.broadcasted_iota(jnp.int32, (18, 768), 0)
    lane = lax.broadcasted_iota(jnp.int32, (18, 768), 1)
    return (lax.rem(row, 6) == lane // 128).astype(F32).astype(BF16)


def pieces(x):
    high = x.astype(BF16).astype(F32)
    rest = x - high
    middle = rest.astype(BF16).astype(F32)
    return [v[:6] for v in (high, middle, rest - middle)]


def flat(x):
    return jnp.concatenate([x[k : k + 1] for k in range(6)], axis=1)


def spread(left, right):
    return lax.dot_general(left.astype(BF16), right, (((0,), (0,)), ((), ())), preferred_element_type=F32)


def differences(on_lanes, on_sublanes, marks):
    left = jnp.concatenate([-v for v in pieces(on_sublanes)] + [jnp.ones((3, 128), F32)], axis=0)
    right = jnp.concatenate([marks] + [flat(v).astype(BF16) for v in pieces(on_lanes)], axis=0)
    return spread(left, right)


def block(x, j, k):
    return x[8 * j : 8 * j + 8, 128 * k : 128 * k + 128]


def stacked(rows):
    return jnp.concatenate([jnp.sum(v, axis=0, keepdims=True) for v in rows] + [jnp.zeros((2, 128), F32)], axis=0)


def pair_force(xa, xb, marks, scale):
    diff = differences(xa, xb, marks)
    rows = []
    for t in range(2):
        acc = [jnp.zeros((8, 128), F32) for _ in range(3)]
        for j in range(16):
            d = [block(diff, j, 3 * t + c) for c in range(3)]
            w = jnp.exp(-0.5 * (d[0] * d[0] + d[1] * d[1] + d[2] * d[2]))
            acc = [acc[c] + w * d[c] for c in range(3)]
        rows += acc
    return scale * stacked(rows)


def pair_adjoint(xa, xb, ga, marks, scale):
    from_a = differences(xa, xb, marks)
    from_b = differences(xb, xa, marks)
    g_sub = spread(jnp.concatenate(pieces(ga), axis=0), marks)
    rows_a, rows_b = [], []
    for t in range(2):
        g = [ga[3 * t + c : 3 * t + c + 1, :] for c in range(3)]
        sum_a = [jnp.zeros((8, 128), F32) for _ in range(3)]
        sum_b = [jnp.zeros((8, 128), F32) for _ in range(3)]
        for j in range(16):
            sum_a = pair_sum(sum_a, [block(from_a, j, 3 * t + c) for c in range(3)], g)
            sum_b = pair_sum(sum_b, [block(from_b, j, 3 * t + c) for c in range(3)], [block(g_sub, j, 3 * t + c) for c in range(3)])
        rows_a += sum_a
        rows_b += sum_b
    return scale * stacked(rows_a), -scale * stacked(rows_b)


def pair_sum(total, d, g):
    w = jnp.exp(-0.5 * (d[0] * d[0] + d[1] * d[1] + d[2] * d[2]))
    s = g[0] * d[0] + g[1] * d[1] + g[2] * d[2]
    return [v + w * (g[c] - s * d[c]) for c, v in enumerate(total)]


def edge_force(own, other, k):
    d = [o - x for o, x in zip(other, own)]
    coef = k * (1.0 - lax.rsqrt(d[0] * d[0] + d[1] * d[1] + d[2] * d[2] + TINY))
    return [coef * e for e in d]


def edge_adjoint(own, other, k, u):
    d = [o - x for o, x in zip(other, own)]
    y = lax.rsqrt(d[0] * d[0] + d[1] * d[1] + d[2] * d[2] + TINY)
    s = d[0] * u[0] + d[1] * u[1] + d[2] * u[2]
    one = 1.0 - y
    k1, k2 = k * one, k * (y * y * y) * s
    return [k1 * u[c] + k2 * d[c] for c in range(3)], one * s


def start_kernel(meta, state, stiff, send_x, send_p, kk):
    first = meta[0, META_C] == 0
    last = meta[0, META_Q] == 63
    column = lax.broadcasted_iota(jnp.int32, (ROWS, COLS), 1)
    kk[0] = jnp.where(column < COLS - 1, stiff[0], 0.0)
    kc = jnp.where(jnp.logical_and(row_is(ROWS - 1), last), 0.0, stiff[1])
    kk[1] = kc
    write_sends(first, [state[t, c] for t in range(2) for c in range(3)], kc, send_x, send_p)


def write_sends(first, values, kc, send_x, send_p):
    tops = jnp.concatenate([v[0:1] for v in values] + [kc[7:8], kc[7:8]], axis=0)
    lows = jnp.concatenate([v[7:8] for v in values] + [kc[7:8], kc[7:8]], axis=0)
    send_x[...] = jnp.where(first, tops, lows)
    send_p[...] = jnp.where(first, lows, tops)


def side_row(first, v, outer):
    return jnp.where(first, v[0:1], v[7:8]) if outer else jnp.where(first, v[7:8], v[0:1])


def forward_inner(step, meta, state, halo_p, kk, force, tiles, acc):
    first = meta[0, META_C] == 0
    row, base = lists(meta, step)
    fill_tiles(tiles, lambda t, c: state[t, c])
    fill_halo(tiles, halo_p[...], halo_p[...])
    acc[...] = jnp.zeros(acc.shape, F32)
    outer = jnp.where(first, 0, EXT - 1)

    count = meta[row, base + 2 * SLOTS]
    marks = selectors()

    def group(i, carry):
        results = []
        for q in range(GROUP):
            p = i * GROUP + q
            a = meta[row, base + p]
            b = meta[row, base + SLOTS + p]
            b_row = b // NB
            live = jnp.logical_and(p < count, b_row != outer)
            at = tile_start(a // NB + 1, lax.rem(a, NB))
            xa = tiles[pl.ds(at, 8), :]
            xb = tiles[pl.ds(tile_start(b_row, lax.rem(b, NB)), 8), :]
            results.append((at, pair_force(xa, xb, marks, jnp.where(live, SCALE, 0.0))))
        for at, value in results:
            acc[pl.ds(at, 8), :] += value
        return carry

    lax.fori_loop(0, (count + GROUP - 1) // GROUP, group, 0)
    kh, kc = kk[0], kk[1]
    k_up = jnp.where(row_is(0), 0.0, pltpu.roll(kc, 1, 0))
    k_side = jnp.where(first, kc[7:8], halo_p[6:7])
    side = jnp.where(first, ROWS - 1, 0)
    for t in range(2):
        x = [state[t, c] for c in range(3)]
        right = edge_force(x, [pltpu.roll(v, COLS - 1, 1) for v in x], kh)
        up = edge_force(x, [pltpu.roll(v, 1, 0) for v in x], k_up)
        edge = edge_force([side_row(first, v, False) for v in x], [halo_p[3 * t + c : 3 * t + c + 1] for c in range(3)], k_side)
        for c in range(3):
            total = right[c] - pltpu.roll(right[c], 1, 1) + up[c] - pltpu.roll(up[c], 7, 0)
            force[3 * t + c] = total + jnp.where(row_is(side), edge[c], 0.0) + read_tiles(acc, 3 * t + c)


def forward_outer(step, meta, state, halo_x, kk, force, state_out, send_x, send_p, tiles, acc, halo):
    first = meta[0, META_C] == 0
    row, base = lists(meta, step)
    count = meta[row, base + 2 * SLOTS]
    outer = jnp.where(first, 0, EXT - 1)
    hits = [jnp.logical_and(p < count, meta[row, base + SLOTS + p] // NB == outer) for p in range(SLOTS)]
    some = functools.reduce(jnp.logical_or, hits)

    @pl.when(some)
    def _():
        acc[...] = jnp.zeros(acc.shape, F32)
        fill_tiles(tiles, lambda t, c: state[t, c])
        for b in range(NB):
            halo[pl.ds(8 * b, 8), :] = halo_x[:, b * 128 : (b + 1) * 128]
        marks = selectors()

        def slot(p, carry):
            a = meta[row, base + p]
            b = meta[row, base + SLOTS + p]

            @pl.when(b // NB == outer)
            def _():
                at = tile_start(a // NB + 1, lax.rem(a, NB))
                xa = tiles[pl.ds(at, 8), :]
                xb = halo[pl.ds(pl.multiple_of(8 * lax.rem(b, NB), 8), 8), :]
                acc[pl.ds(at, 8), :] += pair_force(xa, xb, marks, SCALE)

            return carry

        lax.fori_loop(0, count, slot, 0)
        for k in range(6):
            force[k] = force[k] + read_tiles(acc, k)

    kc = kk[1]
    k_side = jnp.where(first, halo_x[6:7], kc[7:8])
    side = jnp.where(first, 0, ROWS - 1)
    values = []
    for t in range(2):
        x = [state[t, c] for c in range(3)]
        edge = edge_force([side_row(first, v, True) for v in x], [halo_x[3 * t + c : 3 * t + c + 1] for c in range(3)], k_side)
        for c in range(3):
            f = force[3 * t + c] + jnp.where(row_is(side), edge[c], 0.0)
            if c == 2:
                f = f - GRAV
            v = DAMP * (state[t, 3 + c] + H * f)
            new = x[c] + H * v
            state_out[t, c] = new
            state_out[t, 3 + c] = v
            values.append(new)
    write_sends(first, values, kc, send_x, send_p)


def joined(first, lam, got_x, got_p):
    up = jnp.where(first, got_x[...], got_p[...])
    down = jnp.where(first, got_p[...], got_x[...])
    result = []
    for t in range(2):
        for c in range(3):
            k = 3 * t + c
            result.append(lam[t, c] + jnp.where(row_is(0), up[k : k + 1], 0.0) + jnp.where(row_is(7), down[k : k + 1], 0.0))
    return result, down[6:7]


def backward_outer(step, opening, keep, meta, lam, *refs):
    refs = list(refs)
    got = None if opening else (refs.pop(0), refs.pop(0))
    state, halo_x, halo_p, kk, lam_out, send_x, send_p, kd = refs[:8]
    refs = refs[8:]
    full = refs.pop(0) if keep else None
    tiles, grads, acc, acc_b = refs
    first = meta[0, META_C] == 0
    row, base = lists(meta, step)
    count = meta[row, base + 2 * SLOTS]
    if opening:
        xbar = [lam[t, c] for t in range(2) for c in range(3)]
        got_k = jnp.zeros((1, COLS), F32)
    else:
        xbar, got_k = joined(first, lam, *got)
    force = []
    for t in range(2):
        for c in range(3):
            vbar = lam[t, 3 + c]
            if keep:
                full[t, c] = xbar[3 * t + c]
                full[t, 3 + c] = vbar
            a = DAMP * (vbar + H * xbar[3 * t + c])
            lam_out[t, 3 + c] = a
            force.append(H * a)
    up = jnp.where(first, halo_x[...], halo_p[...])
    down = jnp.where(first, halo_p[...], halo_x[...])
    kc = kk[1]
    up_rows, down_rows = [], []
    up_k = jnp.zeros((1, COLS), F32)
    down_k = got_k
    for t in range(2):
        x = [state[t, c] for c in range(3)]
        g = force[3 * t : 3 * t + 3]
        eu, ku = edge_adjoint([v[0:1] for v in x], [up[3 * t + c : 3 * t + c + 1] for c in range(3)], up[6:7], [v[0:1] for v in g])
        ed, kw = edge_adjoint([v[7:8] for v in x], [down[3 * t + c : 3 * t + c + 1] for c in range(3)], kc[7:8], [v[7:8] for v in g])
        up_rows += eu
        down_rows += ed
        up_k = up_k + ku
        down_k = down_k + kw
        for c in range(3):
            lam_out[t, c] = xbar[3 * t + c] - jnp.where(row_is(0), eu[c], 0.0) - jnp.where(row_is(7), ed[c], 0.0)
    kd[...] = jnp.broadcast_to(down_k, (8, COLS))
    zero = jnp.zeros((1, COLS), F32)
    msg_up = jnp.concatenate(up_rows + [up_k, zero], axis=0)
    msg_down = jnp.concatenate(down_rows + [zero, zero], axis=0)
    send_x[...] = jnp.where(first, msg_up, msg_down)
    send_p[...] = jnp.where(first, msg_down, msg_up)

    def far(b):
        return jnp.logical_or(b < NB, b >= NB * (EXT - 1))

    hits = [jnp.logical_and(p < count, far(meta[row, base + SLOTS + p])) for p in range(SLOTS)]
    some = functools.reduce(jnp.logical_or, hits)

    @pl.when(some)
    def _():
        acc[...] = jnp.zeros(acc.shape, F32)
        acc_b[...] = jnp.zeros(acc_b.shape, F32)
        fill_tiles(tiles, lambda t, c: state[t, c])
        fill_halo(tiles, up, down)
        fill_tiles(grads, lambda t, c: force[3 * t + c])
        marks = selectors()

        def slot(p, carry):
            a = meta[row, base + p]
            b = meta[row, base + SLOTS + p]

            @pl.when(far(b))
            def _():
                at = tile_start(a // NB + 1, lax.rem(a, NB))
                bt = tile_start(b // NB, lax.rem(b, NB))
                con_a, con_b = pair_adjoint(tiles[pl.ds(at, 8), :], tiles[pl.ds(bt, 8), :], grads[pl.ds(at, 8), :], marks, SCALE)
                acc[pl.ds(at, 8), :] += con_a
                out = pl.multiple_of(8 * jnp.where(b < NB, b, b - NB * (EXT - 2)), 8)
                acc_b[pl.ds(out, 8), :] += con_b

            return carry

        lax.fori_loop(0, count, slot, 0)
        for t in range(2):
            for c in range(3):
                lam_out[t, c] = lam_out[t, c] + read_tiles(acc, 3 * t + c)
        more_up = jnp.concatenate([acc_b[8 * b : 8 * b + 8, :] for b in range(NB)], axis=1)
        more_down = jnp.concatenate([acc_b[8 * (NB + b) : 8 * (NB + b) + 8, :] for b in range(NB)], axis=1)
        send_x[...] += jnp.where(first, more_up, more_down)
        send_p[...] += jnp.where(first, more_down, more_up)


def backward_inner(step, opening, meta, lam, state, kk, kd, *refs):
    refs = list(refs)
    old = None if opening else refs.pop(0)
    lam_out, grad, tiles, grads, acc = refs
    row, base = lists(meta, step)
    last = meta[0, META_Q] == 63
    fill_tiles(tiles, lambda t, c: state[t, c])
    fill_tiles(grads, lambda t, c: H * lam[t, 3 + c])
    zero = jnp.zeros((8, COLS), F32)
    fill_halo(tiles, zero, zero)
    acc[...] = jnp.zeros(acc.shape, F32)
    count = meta[row, base + 2 * SLOTS]
    marks = selectors()

    def group(i, carry):
        results = []
        for q in range(GROUP):
            p = i * GROUP + q
            a = meta[row, base + p]
            b = meta[row, base + SLOTS + p]
            live = jnp.logical_and(p < count, jnp.logical_and(b >= NB, b < NB * (EXT - 1)))
            at = tile_start(a // NB + 1, lax.rem(a, NB))
            bt = tile_start(b // NB, lax.rem(b, NB))
            scale = jnp.where(live, SCALE, 0.0)
            results.append((at, bt, *pair_adjoint(tiles[pl.ds(at, 8), :], tiles[pl.ds(bt, 8), :], grads[pl.ds(at, 8), :], marks, scale)))
        for at, bt, con_a, con_b in results:
            acc[pl.ds(at, 8), :] += con_a
            acc[pl.ds(bt, 8), :] += con_b
        return carry

    lax.fori_loop(0, (count + GROUP - 1) // GROUP, group, 0)
    kh, kc = kk[0], kk[1]
    k_up = jnp.where(row_is(0), 0.0, pltpu.roll(kc, 1, 0))
    grad_h = jnp.zeros((ROWS, COLS), F32)
    grad_v = jnp.zeros((ROWS, COLS), F32)
    for t in range(2):
        x = [state[t, c] for c in range(3)]
        g = [H * lam[t, 3 + c] for c in range(3)]
        right, rk = edge_adjoint(x, [pltpu.roll(v, COLS - 1, 1) for v in x], kh, [v - pltpu.roll(v, COLS - 1, 1) for v in g])
        up, uk = edge_adjoint(x, [pltpu.roll(v, 1, 0) for v in x], k_up, [v - pltpu.roll(v, 1, 0) for v in g])
        grad_h = grad_h + rk
        grad_v = grad_v + uk
        for c in range(3):
            total = pltpu.roll(right[c], 1, 1) - right[c] + pltpu.roll(up[c], 7, 0) - up[c]
            lam_out[t, c] = lam[t, c] + total + read_tiles(acc, 3 * t + c)
            lam_out[t, 3 + c] = lam[t, 3 + c]
    column = lax.broadcasted_iota(jnp.int32, (ROWS, COLS), 1)
    grad_h = jnp.where(column < COLS - 1, grad_h, 0.0)
    grad_v = jnp.where(row_is(7), jnp.where(last, 0.0, kd[0:1]), pltpu.roll(grad_v, 7, 0))
    if opening:
        grad[0] = grad_h
        grad[1] = grad_v
    else:
        grad[0] = old[0] + grad_h
        grad[1] = old[1] + grad_v


def end_kernel(meta, lam, got_x, got_p, old, out):
    first = meta[0, META_C] == 0
    last = meta[0, META_Q] == 63
    xbar, got_k = joined(first, lam, got_x, got_p)
    zero = jnp.zeros((2, COLS), F32)
    tops = jnp.concatenate([v[0:1] for v in xbar] + [zero], axis=0)
    lows = jnp.concatenate([v[7:8] for v in xbar] + [zero], axis=0)
    below = old[1] + jnp.where(row_is(7), jnp.where(last, 0.0, got_k), 0.0)
    for s in range(out.shape[0]):
        out[s, 0] = old[0]
        out[s, 1] = below
        out[s, 2] = tops
        out[s, 3] = lows


def output_kernel(meta, swapped, shared, *refs):
    *lams, adjoint, grad = refs
    here = meta[0, META_S] == 0
    for k in range(2):
        grad[k] = shared[0, k] + shared[1, k] + shared[2, k] + shared[3, k]

    @pl.when(here)
    def _():
        for s, lam in enumerate(lams):
            for t in range(2):
                for c in range(3):
                    k = 3 * t + c
                    v = jnp.where(row_is(0), shared[s, 2, k : k + 1], lam[t, c])
                    adjoint[s, t, c] = jnp.where(row_is(7), shared[s, 3, k : k + 1], v)
                    adjoint[s, t, 3 + c] = lam[t, 3 + c]

    @pl.when(jnp.logical_not(here))
    def _():
        adjoint[...] = swapped[...]


STATE = jax.ShapeDtypeStruct((2, 6, ROWS, COLS), F32)
HALO = jax.ShapeDtypeStruct((8, COLS), F32)
GRADS = jax.ShapeDtypeStruct((2, ROWS, COLS), F32)
TILES = pltpu.VMEM((EXT * NB * 8, 128), F32)
SMALL = pltpu.VMEM((NB * 8, 128), F32)


def call(body, outs, operands, scratch=(), flops=0, placed=True):
    spaces = [pltpu.VMEM if k else pltpu.SMEM for k in range(len(operands))]
    if placed:
        operands = [pltpu.with_memory_space_constraint(x, space) for x, space in zip(operands, spaces)]
        outs = [pltpu.VMEM(o.shape, o.dtype) for o in outs]
    return pl.pallas_call(
        body,
        out_shape=outs,
        in_specs=[pl.BlockSpec(memory_space=space) for space in spaces],
        out_specs=[pl.BlockSpec(memory_space=pltpu.VMEM)] * len(outs),
        scratch_shapes=list(scratch),
        cost_estimate=pl.CostEstimate(flops=flops, transcendentals=0, bytes_accessed=1 << 18) if flops else None,
    )(*operands)


def on_device(start_state, stiffness, contact_a, contact_b, pair_count, cotangent):
    section = lax.axis_index("section")
    space = lax.axis_index("space")
    sections = lax.axis_size("section")
    spaces = lax.axis_size("space")
    cross = [(i, i + 1) for i in range(1, spaces - 1, 2)]
    cross = cross + [(b, a) for a, b in cross]
    near = [(i, i ^ 1) for i in range(spaces)]
    steps = contact_a.shape[0] * sections

    facts = jnp.stack([section, lax.rem(space, 2), space]).astype(jnp.int32)
    own_list = jnp.concatenate(
        [
            contact_a[:, 0],
            contact_b[:, 0],
            jnp.broadcast_to(pair_count, (2, 8)),
            jnp.broadcast_to(jnp.pad(facts, (0, 5)), (2, 8)),
        ],
        axis=1,
    ).reshape(1, 64)
    others = [lax.ppermute(own_list, "section", [(i, (i + k) % sections) for i in range(sections)]) for k in range(1, sections)]
    meta = jnp.concatenate([own_list] + others, axis=0)

    state = lax.dynamic_slice_in_dim(start_state, section * 2, 2, 0)
    lam = lax.dynamic_slice_in_dim(cotangent, section * 2, 2, 0)
    send_x, send_p, kk = call(start_kernel, [HALO, HALO, GRADS], [own_list, state, stiffness])

    states, halos, exits = [], [], []
    for step in range(steps):
        halo_x = lax.ppermute(send_x, "space", cross)
        halo_p = lax.ppermute(send_p, "space", near)
        (force,) = call(
            functools.partial(forward_inner, step),
            [jax.ShapeDtypeStruct((6, ROWS, COLS), F32)],
            [meta, state, halo_p, kk],
            [TILES, TILES],
            flops=4000000,
        )
        states.append(state)
        halos.append((halo_x, halo_p))
        state, send_x, send_p = call(
            functools.partial(forward_outer, step), [STATE, HALO, HALO], [meta, state, halo_x, kk, force], [TILES, TILES, SMALL]
        )
        if step % 2 == 1:
            exits.append(state)
    exit_state = lax.all_to_all(jnp.stack(exits), "section", 0, 0, tiled=True)

    grad = None
    got = ()
    fulls = {}
    for step in reversed(range(steps)):
        opening = step == steps - 1
        keep = step % 2 == 1 and not opening
        outs = [STATE, HALO, HALO, HALO] + ([STATE] if keep else [])
        lam, send_x, send_p, kd, *rest = call(
            functools.partial(backward_outer, step, opening, keep),
            outs,
            [meta, lam, *got, states[step], *halos[step], kk],
            [TILES, TILES, TILES, pltpu.VMEM((2 * NB * 8, 128), F32)],
        )
        if keep:
            fulls[(step + 1) // 2] = rest[0]
        got = (lax.ppermute(send_x, "space", cross), lax.ppermute(send_p, "space", near))
        lam, grad = call(
            functools.partial(backward_inner, step, opening),
            [STATE, GRADS],
            [meta, lam, states[step], kk, kd] + ([] if opening else [grad]),
            [TILES, TILES, TILES],
            flops=8000000,
        )
        if step == 1:
            swapped = lax.all_to_all(jnp.stack([fulls[max(s, 1)] for s in range(sections)]), "section", 0, 0, tiled=True)
    lams = [lam]
    for s in range(1, sections):
        lams.append(lax.ppermute(lam, "section", [(s, 0)]))
    (shared,) = call(end_kernel, [jax.ShapeDtypeStruct((sections, 4, ROWS, COLS), F32)], [meta, lam, *got, grad])
    shared = lax.all_to_all(shared, "section", 0, 0, tiled=True)
    adjoint, stiffness_grad = call(
        output_kernel, [jax.ShapeDtypeStruct((sections, 2, 6, ROWS, COLS), F32), GRADS], [meta, swapped, shared, *lams], placed=False
    )
    return (
        exit_state.reshape(1, 8, 6, ROWS, COLS),
        adjoint.reshape(1, 8, 6, ROWS, COLS),
        stiffness_grad,
    )


def solution(mesh):
    in_specs = (
        P(None, None, "space", None),
        P(None, "space", None),
        P("section", "space", None),
        P("section", "space", None),
        P("section", "space"),
        P(None, None, "space", None),
    )
    out_specs = (
        P("section", None, None, "space", None),
        P("section", None, None, "space", None),
        P(None, "space", None),
    )
    return jax.shard_map(on_device, mesh=mesh, in_specs=in_specs, out_specs=out_specs, check_vma=False)
```

```python
import functools

import jax
import jax.numpy as jnp
from jax import lax
from jax.experimental import pallas as pl
from jax.experimental.pallas import tpu as pltpu
from jax.sharding import PartitionSpec as P


H = 0.1
DAMP = 0.98
SCALE = 0.3
GRAV = 0.5
TINY = 1e-06
F32 = jnp.float32
BF16 = jnp.bfloat16
COPY_STEP = 3
GROUP = 2
SLOTS = 8
ROWS = 8
COLS = 512
NB = COLS // 128
EXT = ROWS + 2
META_S, META_C, META_Q = 24, 25, 26


def lists(meta, step):
    section = meta[0, META_S]
    row = lax.rem(section - step // 2 + 4, 4)
    base = 32 * (step % 2)
    return row, base


def tile_start(row, block):
    return pl.multiple_of((block * EXT + row) * 8, 8)


def row_is(r, n=COLS):
    return lax.broadcasted_iota(jnp.int32, (ROWS, n), 0) == r


def fill_tiles(tiles, value_of):
    for t in range(2):
        for c in range(3):
            v = value_of(t, c)
            for b in range(NB):
                tiles[pl.ds((b * EXT + 1) * 8 + 3 * t + c, ROWS, stride=8), :] = v[:, b * 128 : (b + 1) * 128]


def read_tiles(tiles, k):
    return jnp.concatenate([tiles[pl.ds((b * EXT + 1) * 8 + k, ROWS, stride=8), :] for b in range(NB)], axis=1)


def fill_halo(tiles, up, down):
    for b in range(NB):
        tiles[pl.ds(b * EXT * 8, 8), :] = up[:, b * 128 : (b + 1) * 128]
        tiles[pl.ds((b * EXT + EXT - 1) * 8, 8), :] = down[:, b * 128 : (b + 1) * 128]


def selectors():
    row = lax.broadcasted_iota(jnp.int32, (18, 768), 0)
    lane = lax.broadcasted_iota(jnp.int32, (18, 768), 1)
    return (lax.rem(row, 6) == lane // 128).astype(F32).astype(BF16)


def pieces(x):
    high = x.astype(BF16).astype(F32)
    rest = x - high
    middle = rest.astype(BF16).astype(F32)
    return [v[:6] for v in (high, middle, rest - middle)]


def flat(x):
    return jnp.concatenate([x[k : k + 1] for k in range(6)], axis=1)


def spread(left, right):
    return lax.dot_general(left.astype(BF16), right, (((0,), (0,)), ((), ())), preferred_element_type=F32)


def differences(on_lanes, on_sublanes, marks):
    left = jnp.concatenate([-v for v in pieces(on_sublanes)] + [jnp.ones((3, 128), F32)], axis=0)
    right = jnp.concatenate([marks] + [flat(v).astype(BF16) for v in pieces(on_lanes)], axis=0)
    return spread(left, right)


def block(x, j, k):
    return x[8 * j : 8 * j + 8, 128 * k : 128 * k + 128]


def stacked(rows):
    return jnp.concatenate([jnp.sum(v, axis=0, keepdims=True) for v in rows] + [jnp.zeros((2, 128), F32)], axis=0)


def pair_force(xa, xb, marks, scale):
    diff = differences(xa, xb, marks)
    rows = []
    for t in range(2):
        acc = [jnp.zeros((8, 128), F32) for _ in range(3)]
        for j in range(16):
            d = [block(diff, j, 3 * t + c) for c in range(3)]
            w = jnp.exp(-0.5 * (d[0] * d[0] + d[1] * d[1] + d[2] * d[2]))
            acc = [acc[c] + w * d[c] for c in range(3)]
        rows += acc
    return scale * stacked(rows)


def pair_adjoint(xa, xb, ga, marks, scale_a, scale_b):
    from_a = differences(xa, xb, marks) if scale_a is not None else None
    from_b = differences(xb, xa, marks)
    g_sub = spread(jnp.concatenate(pieces(ga), axis=0), marks)
    rows_a, rows_b = [], []
    for t in range(2):
        g = [ga[3 * t + c : 3 * t + c + 1, :] for c in range(3)]
        sum_a = [jnp.zeros((8, 128), F32) for _ in range(3)]
        sum_b = [jnp.zeros((8, 128), F32) for _ in range(3)]
        for j in range(16):
            if scale_a is not None:
                sum_a = pair_sum(sum_a, [block(from_a, j, 3 * t + c) for c in range(3)], g)
            sum_b = pair_sum(sum_b, [block(from_b, j, 3 * t + c) for c in range(3)], [block(g_sub, j, 3 * t + c) for c in range(3)])
        rows_a += sum_a
        rows_b += sum_b
    con_a = scale_a * stacked(rows_a) if scale_a is not None else None
    return con_a, -scale_b * stacked(rows_b)


def pair_sum(total, d, g):
    w = jnp.exp(-0.5 * (d[0] * d[0] + d[1] * d[1] + d[2] * d[2]))
    s = g[0] * d[0] + g[1] * d[1] + g[2] * d[2]
    return [v + w * (g[c] - s * d[c]) for c, v in enumerate(total)]


def edge_force(own, other, k):
    d = [o - x for o, x in zip(other, own)]
    coef = k * (1.0 - lax.rsqrt(d[0] * d[0] + d[1] * d[1] + d[2] * d[2] + TINY))
    return [coef * e for e in d]


def edge_adjoint(own, other, k, u):
    d = [o - x for o, x in zip(other, own)]
    y = lax.rsqrt(d[0] * d[0] + d[1] * d[1] + d[2] * d[2] + TINY)
    s = d[0] * u[0] + d[1] * u[1] + d[2] * u[2]
    one = 1.0 - y
    k1, k2 = k * one, k * (y * y * y) * s
    return [k1 * u[c] + k2 * d[c] for c in range(3)], one * s


def start_kernel(meta, state, stiff, send_x, send_p, kk):
    first = meta[0, META_C] == 0
    last = meta[0, META_Q] == 63
    column = lax.broadcasted_iota(jnp.int32, (ROWS, COLS), 1)
    kk[0] = jnp.where(column < COLS - 1, stiff[0], 0.0)
    kc = jnp.where(jnp.logical_and(row_is(ROWS - 1), last), 0.0, stiff[1])
    kk[1] = kc
    write_sends(first, [state[t, c] for t in range(2) for c in range(3)], kc, send_x, send_p)


def write_sends(first, values, kc, send_x, send_p):
    tops = jnp.concatenate([v[0:1] for v in values] + [kc[7:8], kc[7:8]], axis=0)
    lows = jnp.concatenate([v[7:8] for v in values] + [kc[7:8], kc[7:8]], axis=0)
    send_x[...] = jnp.where(first, tops, lows)
    send_p[...] = jnp.where(first, lows, tops)


def side_row(first, v, outer):
    return jnp.where(first, v[0:1], v[7:8]) if outer else jnp.where(first, v[7:8], v[0:1])


def forward_inner(step, meta, state, halo_p, kk, force, tiles, acc):
    first = meta[0, META_C] == 0
    row, base = lists(meta, step)
    fill_tiles(tiles, lambda t, c: state[t, c])
    fill_halo(tiles, halo_p[...], halo_p[...])
    acc[...] = jnp.zeros(acc.shape, F32)
    outer = jnp.where(first, 0, EXT - 1)

    count = meta[row, base + 2 * SLOTS]
    marks = selectors()

    def group(i, carry):
        results = []
        for q in range(GROUP):
            p = i * GROUP + q
            a = meta[row, base + p]
            b = meta[row, base + SLOTS + p]
            b_row = b // NB
            live = jnp.logical_and(p < count, b_row != outer)
            at = tile_start(a // NB + 1, lax.rem(a, NB))
            xa = tiles[pl.ds(at, 8), :]
            xb = tiles[pl.ds(tile_start(b_row, lax.rem(b, NB)), 8), :]
            results.append((at, pair_force(xa, xb, marks, jnp.where(live, SCALE, 0.0))))
        for at, value in results:
            acc[pl.ds(at, 8), :] += value
        return carry

    lax.fori_loop(0, (count + GROUP - 1) // GROUP, group, 0)
    kh, kc = kk[0], kk[1]
    k_up = jnp.where(row_is(0), 0.0, pltpu.roll(kc, 1, 0))
    k_side = jnp.where(first, kc[7:8], halo_p[6:7])
    side = jnp.where(first, ROWS - 1, 0)
    for t in range(2):
        x = [state[t, c] for c in range(3)]
        right = edge_force(x, [pltpu.roll(v, COLS - 1, 1) for v in x], kh)
        up = edge_force(x, [pltpu.roll(v, 1, 0) for v in x], k_up)
        edge = edge_force([side_row(first, v, False) for v in x], [halo_p[3 * t + c : 3 * t + c + 1] for c in range(3)], k_side)
        for c in range(3):
            total = right[c] - pltpu.roll(right[c], 1, 1) + up[c] - pltpu.roll(up[c], 7, 0)
            force[3 * t + c] = total + jnp.where(row_is(side), edge[c], 0.0) + read_tiles(acc, 3 * t + c)


def forward_outer(step, meta, state, halo_x, kk, force, state_out, send_x, send_p, tiles, acc, halo):
    first = meta[0, META_C] == 0
    row, base = lists(meta, step)
    count = meta[row, base + 2 * SLOTS]
    outer = jnp.where(first, 0, EXT - 1)
    hits = [jnp.logical_and(p < count, meta[row, base + SLOTS + p] // NB == outer) for p in range(SLOTS)]
    some = functools.reduce(jnp.logical_or, hits)

    @pl.when(some)
    def _():
        acc[...] = jnp.zeros(acc.shape, F32)
        fill_tiles(tiles, lambda t, c: state[t, c])
        for b in range(NB):
            halo[pl.ds(8 * b, 8), :] = halo_x[:, b * 128 : (b + 1) * 128]
        marks = selectors()

        def slot(p, carry):
            a = meta[row, base + p]
            b = meta[row, base + SLOTS + p]

            @pl.when(b // NB == outer)
            def _():
                at = tile_start(a // NB + 1, lax.rem(a, NB))
                xa = tiles[pl.ds(at, 8), :]
                xb = halo[pl.ds(pl.multiple_of(8 * lax.rem(b, NB), 8), 8), :]
                acc[pl.ds(at, 8), :] += pair_force(xa, xb, marks, SCALE)

            return carry

        lax.fori_loop(0, count, slot, 0)
        for k in range(6):
            force[k] = force[k] + read_tiles(acc, k)

    kc = kk[1]
    k_side = jnp.where(first, halo_x[6:7], kc[7:8])
    side = jnp.where(first, 0, ROWS - 1)
    values = []
    for t in range(2):
        x = [state[t, c] for c in range(3)]
        edge = edge_force([side_row(first, v, True) for v in x], [halo_x[3 * t + c : 3 * t + c + 1] for c in range(3)], k_side)
        for c in range(3):
            f = force[3 * t + c] + jnp.where(row_is(side), edge[c], 0.0)
            if c == 2:
                f = f - GRAV
            v = DAMP * (state[t, 3 + c] + H * f)
            new = x[c] + H * v
            state_out[t, c] = new
            state_out[t, 3 + c] = v
            values.append(new)
    write_sends(first, values, kc, send_x, send_p)


def joined(first, lam, got_x, got_p):
    up = jnp.where(first, got_x[...], got_p[...])
    down = jnp.where(first, got_p[...], got_x[...])
    result = []
    for t in range(2):
        for c in range(3):
            k = 3 * t + c
            result.append(lam[t, c] + jnp.where(row_is(0), up[k : k + 1], 0.0) + jnp.where(row_is(7), down[k : k + 1], 0.0))
    return result, down[6:7]


def backward_outer(step, opening, keep, meta, lam, *refs):
    refs = list(refs)
    got = None if opening else (refs.pop(0), refs.pop(0))
    state, halo_x, halo_p, kk, lam_out, send_x, send_p, kd = refs[:8]
    refs = refs[8:]
    full = refs.pop(0) if keep else None
    tiles, grads, acc_b = refs
    first = meta[0, META_C] == 0
    row, base = lists(meta, step)
    count = meta[row, base + 2 * SLOTS]
    if opening:
        xbar = [lam[t, c] for t in range(2) for c in range(3)]
        got_k = jnp.zeros((1, COLS), F32)
    else:
        xbar, got_k = joined(first, lam, *got)
    force = []
    for t in range(2):
        for c in range(3):
            vbar = lam[t, 3 + c]
            if keep:
                full[t, c] = xbar[3 * t + c]
                full[t, 3 + c] = vbar
            a = DAMP * (vbar + H * xbar[3 * t + c])
            lam_out[t, 3 + c] = a
            force.append(H * a)
    up = jnp.where(first, halo_x[...], halo_p[...])
    down = jnp.where(first, halo_p[...], halo_x[...])
    kc = kk[1]
    up_rows, down_rows = [], []
    up_k = jnp.zeros((1, COLS), F32)
    down_k = got_k
    for t in range(2):
        x = [state[t, c] for c in range(3)]
        g = force[3 * t : 3 * t + 3]
        eu, ku = edge_adjoint([v[0:1] for v in x], [up[3 * t + c : 3 * t + c + 1] for c in range(3)], up[6:7], [v[0:1] for v in g])
        ed, kw = edge_adjoint([v[7:8] for v in x], [down[3 * t + c : 3 * t + c + 1] for c in range(3)], kc[7:8], [v[7:8] for v in g])
        up_rows += eu
        down_rows += ed
        up_k = up_k + ku
        down_k = down_k + kw
        for c in range(3):
            lam_out[t, c] = xbar[3 * t + c] - jnp.where(row_is(0), eu[c], 0.0) - jnp.where(row_is(7), ed[c], 0.0)
    kd[...] = jnp.broadcast_to(down_k, (8, COLS))
    zero = jnp.zeros((1, COLS), F32)
    msg_up = jnp.concatenate(up_rows + [up_k, zero], axis=0)
    msg_down = jnp.concatenate(down_rows + [zero, zero], axis=0)
    send_x[...] = jnp.where(first, msg_up, msg_down)
    send_p[...] = jnp.where(first, msg_down, msg_up)

    def far(b):
        return jnp.logical_or(b < NB, b >= NB * (EXT - 1))

    hits = [jnp.logical_and(p < count, far(meta[row, base + SLOTS + p])) for p in range(SLOTS)]
    some = functools.reduce(jnp.logical_or, hits)

    @pl.when(some)
    def _():
        acc_b[...] = jnp.zeros(acc_b.shape, F32)
        fill_tiles(tiles, lambda t, c: state[t, c])
        fill_halo(tiles, up, down)
        fill_tiles(grads, lambda t, c: force[3 * t + c])
        marks = selectors()

        def slot(p, carry):
            a = meta[row, base + p]
            b = meta[row, base + SLOTS + p]

            @pl.when(far(b))
            def _():
                at = tile_start(a // NB + 1, lax.rem(a, NB))
                bt = tile_start(b // NB, lax.rem(b, NB))
                _, con_b = pair_adjoint(tiles[pl.ds(at, 8), :], tiles[pl.ds(bt, 8), :], grads[pl.ds(at, 8), :], marks, None, SCALE)
                out = pl.multiple_of(8 * jnp.where(b < NB, b, b - NB * (EXT - 2)), 8)
                acc_b[pl.ds(out, 8), :] += con_b

            return carry

        lax.fori_loop(0, count, slot, 0)
        more_up = jnp.concatenate([acc_b[8 * b : 8 * b + 8, :] for b in range(NB)], axis=1)
        more_down = jnp.concatenate([acc_b[8 * (NB + b) : 8 * (NB + b) + 8, :] for b in range(NB)], axis=1)
        send_x[...] += jnp.where(first, more_up, more_down)
        send_p[...] += jnp.where(first, more_down, more_up)


def backward_inner(step, opening, meta, lam, state, halo_x, halo_p, kk, kd, *refs):
    refs = list(refs)
    old = None if opening else refs.pop(0)
    copies = []
    if step == COPY_STEP:
        source, target, sems = refs.pop(0), refs.pop(2), refs.pop()
        copies = [pltpu.make_async_copy(source.at[s], target.at[s], sems.at[s]) for s in range(4)]
        for copy in copies:
            copy.start()
    lam_out, grad, tiles, grads, acc = refs
    row, base = lists(meta, step)
    last = meta[0, META_Q] == 63
    fill_tiles(tiles, lambda t, c: state[t, c])
    fill_tiles(grads, lambda t, c: H * lam[t, 3 + c])
    first = meta[0, META_C] == 0
    fill_halo(tiles, jnp.where(first, halo_x[...], halo_p[...]), jnp.where(first, halo_p[...], halo_x[...]))
    acc[...] = jnp.zeros(acc.shape, F32)
    count = meta[row, base + 2 * SLOTS]
    marks = selectors()

    def group(i, carry):
        results = []
        for q in range(GROUP):
            p = i * GROUP + q
            a = meta[row, base + p]
            b = meta[row, base + SLOTS + p]
            live = p < count
            inside = jnp.logical_and(live, jnp.logical_and(b >= NB, b < NB * (EXT - 1)))
            at = tile_start(a // NB + 1, lax.rem(a, NB))
            bt = tile_start(b // NB, lax.rem(b, NB))
            scales = [jnp.where(on, SCALE, 0.0) for on in (live, inside)]
            results.append((at, bt, *pair_adjoint(tiles[pl.ds(at, 8), :], tiles[pl.ds(bt, 8), :], grads[pl.ds(at, 8), :], marks, *scales)))
        for at, bt, con_a, con_b in results:
            acc[pl.ds(at, 8), :] += con_a
            acc[pl.ds(bt, 8), :] += con_b
        return carry

    lax.fori_loop(0, (count + GROUP - 1) // GROUP, group, 0)
    kh, kc = kk[0], kk[1]
    k_up = jnp.where(row_is(0), 0.0, pltpu.roll(kc, 1, 0))
    grad_h = jnp.zeros((ROWS, COLS), F32)
    grad_v = jnp.zeros((ROWS, COLS), F32)
    for t in range(2):
        x = [state[t, c] for c in range(3)]
        g = [H * lam[t, 3 + c] for c in range(3)]
        right, rk = edge_adjoint(x, [pltpu.roll(v, COLS - 1, 1) for v in x], kh, [v - pltpu.roll(v, COLS - 1, 1) for v in g])
        up, uk = edge_adjoint(x, [pltpu.roll(v, 1, 0) for v in x], k_up, [v - pltpu.roll(v, 1, 0) for v in g])
        grad_h = grad_h + rk
        grad_v = grad_v + uk
        for c in range(3):
            total = pltpu.roll(right[c], 1, 1) - right[c] + pltpu.roll(up[c], 7, 0) - up[c]
            lam_out[t, c] = lam[t, c] + total + read_tiles(acc, 3 * t + c)
            lam_out[t, 3 + c] = lam[t, 3 + c]
    column = lax.broadcasted_iota(jnp.int32, (ROWS, COLS), 1)
    grad_h = jnp.where(column < COLS - 1, grad_h, 0.0)
    grad_v = jnp.where(row_is(7), jnp.where(last, 0.0, kd[0:1]), pltpu.roll(grad_v, 7, 0))
    if opening:
        grad[0] = grad_h
        grad[1] = grad_v
    else:
        grad[0] = old[0] + grad_h
        grad[1] = old[1] + grad_v
    for copy in copies:
        copy.wait()


def end_kernel(meta, lam, got_x, got_p, old, out):
    first = meta[0, META_C] == 0
    last = meta[0, META_Q] == 63
    xbar, got_k = joined(first, lam, got_x, got_p)
    zero = jnp.zeros((2, COLS), F32)
    out[0] = old[0]
    out[1] = old[1] + jnp.where(row_is(7), jnp.where(last, 0.0, got_k), 0.0)
    out[2] = jnp.concatenate([v[0:1] for v in xbar] + [zero], axis=0)
    out[3] = jnp.concatenate([v[7:8] for v in xbar] + [zero], axis=0)


def output_kernel(sections, meta, swapped, *refs):
    shared, lams = refs[:sections], refs[sections : 2 * sections]
    adjoint, grad, buffer, total, sems = refs[2 * sections :]
    here = meta[0, META_S] == 0

    @pl.when(jnp.logical_not(here))
    def _():
        for s in range(sections):
            pltpu.make_async_copy(swapped.at[s], adjoint.at[s], sems.at[s]).start()

    @pl.when(here)
    def _():
        for s, lam in enumerate(lams):
            part = shared[-s % sections]
            for t in range(2):
                for c in range(3):
                    k = 3 * t + c
                    v = jnp.where(row_is(0), part[2, k : k + 1], lam[t, c])
                    buffer[s, t, c] = jnp.where(row_is(7), part[3, k : k + 1], v)
                    buffer[s, t, 3 + c] = lam[t, 3 + c]
            pltpu.make_async_copy(buffer.at[s], adjoint.at[s], sems.at[s]).start()

    for own in range(sections):

        @pl.when(meta[0, META_S] == own)
        def _(own=own):
            for k in range(2):
                value = shared[own % sections][k]
                for s in range(1, sections):
                    value = value + shared[(own - s) % sections][k]
                total[k] = value

    last = pltpu.make_async_copy(total, grad, sems.at[sections])
    last.start()
    for s in range(sections):
        pltpu.make_async_copy(buffer.at[s], adjoint.at[s], sems.at[s]).wait()
    last.wait()


STATE = jax.ShapeDtypeStruct((2, 6, ROWS, COLS), F32)
HALO = jax.ShapeDtypeStruct((8, COLS), F32)
CHUNKS = jax.ShapeDtypeStruct((4, 2, 6, ROWS, COLS), F32)
GRADS = jax.ShapeDtypeStruct((2, ROWS, COLS), F32)
TILES = pltpu.VMEM((EXT * NB * 8, 128), F32)
SMALL = pltpu.VMEM((NB * 8, 128), F32)


def call(body, outs, operands, scratch=(), flops=0, hbm_out=()):
    spaces = [pltpu.VMEM if k else pltpu.SMEM for k in range(len(operands))]
    operands = [pltpu.with_memory_space_constraint(x, space) for x, space in zip(operands, spaces)]
    out_spaces = [pltpu.HBM if k in hbm_out else pltpu.VMEM for k in range(len(outs))]
    return pl.pallas_call(
        body,
        out_shape=[space(o.shape, o.dtype) for space, o in zip(out_spaces, outs)],
        in_specs=[pl.BlockSpec(memory_space=space) for space in spaces],
        out_specs=[pl.BlockSpec(memory_space=space) for space in out_spaces],
        scratch_shapes=list(scratch),
        cost_estimate=pl.CostEstimate(flops=flops, transcendentals=0, bytes_accessed=1 << 18) if flops else None,
    )(*operands)


def on_device(start_state, stiffness, contact_a, contact_b, pair_count, cotangent):
    section = lax.axis_index("section")
    space = lax.axis_index("space")
    sections = lax.axis_size("section")
    spaces = lax.axis_size("space")
    cross = [(i, i + 1) for i in range(1, spaces - 1, 2)]
    cross = cross + [(b, a) for a, b in cross]
    near = [(i, i ^ 1) for i in range(spaces)]
    steps = contact_a.shape[0] * sections

    facts = jnp.stack([section, lax.rem(space, 2), space]).astype(jnp.int32)
    own_list = jnp.concatenate(
        [
            contact_a[:, 0],
            contact_b[:, 0],
            jnp.broadcast_to(pair_count, (2, 8)),
            jnp.broadcast_to(jnp.pad(facts, (0, 5)), (2, 8)),
        ],
        axis=1,
    ).reshape(1, 64)
    others = [lax.ppermute(own_list, "section", [(i, (i + k) % sections) for i in range(sections)]) for k in range(1, sections)]
    meta = jnp.concatenate([own_list] + others, axis=0)

    state = lax.dynamic_slice_in_dim(start_state, section * 2, 2, 0)
    lam = lax.dynamic_slice_in_dim(cotangent, section * 2, 2, 0)
    send_x, send_p, kk = call(start_kernel, [HALO, HALO, GRADS], [own_list, state, stiffness])

    def exchange(send_x, send_p):
        got_x = lax.ppermute(send_x, "space", cross)
        got_p = lax.ppermute(send_p, "space", near)
        return got_x, got_p

    states, halos, exits = [], [], []
    for step in range(steps):
        halo_x, halo_p = exchange(send_x, send_p)
        (force,) = call(
            functools.partial(forward_inner, step),
            [jax.ShapeDtypeStruct((6, ROWS, COLS), F32)],
            [meta, state, halo_p, kk],
            [TILES, TILES],
            flops=4000000,
        )
        states.append(state)
        halos.append((halo_x, halo_p))
        state, send_x, send_p = call(
            functools.partial(forward_outer, step), [STATE, HALO, HALO], [meta, state, halo_x, kk, force], [TILES, TILES, SMALL]
        )
        if step % 2 == 1:
            exits.append(state)
    exit_state = lax.all_to_all(jnp.stack(exits), "section", 0, 0, tiled=True)

    grad = None
    got = ()
    fulls = []
    for step in reversed(range(steps)):
        opening = step == steps - 1
        keep = step % 2 == 1 and not opening
        lam, send_x, send_p, kd, *rest = call(
            functools.partial(backward_outer, step, opening, keep),
            [STATE, HALO, HALO, HALO] + [STATE] * keep,
            [meta, lam, *got, states[step], *halos[step], kk],
            [TILES, TILES, pltpu.VMEM((2 * NB * 8, 128), F32)],
        )
        fulls = rest + fulls
        got = exchange(send_x, send_p)
        copying = step == COPY_STEP
        operands = [meta, lam, states[step], *halos[step], kk, kd] + ([] if opening else [grad])
        lam, grad, *rest = call(
            functools.partial(backward_inner, step, opening),
            [STATE, GRADS] + [CHUNKS] * copying,
            operands + [exit_state] * copying,
            [TILES, TILES, TILES] + [pltpu.SemaphoreType.DMA((4,))] * copying,
            flops=8000000,
            hbm_out=(2,),
        )
        if copying:
            (exit_state,) = rest
        if step == 1:
            swapped = lax.all_to_all(jnp.stack([fulls[0], *fulls]), "section", 0, 0, tiled=True)
    lams = [lam]
    for s in range(1, sections):
        lams.append(lax.ppermute(lam, "section", [(s, 0)]))
    (shared,) = call(end_kernel, [jax.ShapeDtypeStruct((4, ROWS, COLS), F32)], [meta, lam, *got, grad])
    parts = [shared] + [lax.ppermute(shared, "section", [(i, (i + k) % sections) for i in range(sections)]) for k in range(1, sections)]
    adjoint, stiffness_grad = call(
        functools.partial(output_kernel, sections),
        [CHUNKS, GRADS],
        [meta, swapped, *parts, *lams],
        [pltpu.VMEM((4, 2, 6, ROWS, COLS), F32), pltpu.VMEM((2, ROWS, COLS), F32), pltpu.SemaphoreType.DMA((5,))],
        hbm_out=(0, 1),
    )
    return (
        exit_state.reshape(1, 8, 6, ROWS, COLS),
        adjoint.reshape(1, 8, 6, ROWS, COLS),
        stiffness_grad,
    )


def solution(mesh):
    in_specs = (
        P(None, None, "space", None),
        P(None, "space", None),
        P("section", "space", None),
        P("section", "space", None),
        P("section", "space"),
        P(None, None, "space", None),
    )
    out_specs = (
        P("section", None, None, "space", None),
        P("section", None, None, "space", None),
        P(None, "space", None),
    )
    return jax.shard_map(on_device, mesh=mesh, in_specs=in_specs, out_specs=out_specs, check_vma=False)
```

```python
import functools

import jax
import jax.numpy as jnp
from jax import lax
from jax.experimental import pallas as pl
from jax.experimental.pallas import tpu as pltpu
from jax.sharding import PartitionSpec as P


H = 0.1
DAMP = 0.98
SCALE = 0.3
GRAV = 0.5
TINY = 1e-06
F32 = jnp.float32
BF16 = jnp.bfloat16
COPY_STEP = 3
GROUP = 2
GROUP_BACK = 2
SLOTS = 8
ROWS = 8
COLS = 512
NB = COLS // 128
EXT = ROWS + 2
META_S, META_C, META_Q = 24, 25, 26


def lists(meta, step):
    section = meta[0, META_S]
    row = lax.rem(section - step // 2 + 4, 4)
    base = 32 * (step % 2)
    return row, base


def tile_start(row, block):
    return pl.multiple_of((block * EXT + row) * 8, 8)


def row_is(r, n=COLS):
    return lax.broadcasted_iota(jnp.int32, (ROWS, n), 0) == r


def fill_tiles(tiles, value_of):
    for t in range(2):
        for c in range(3):
            v = value_of(t, c)
            for b in range(NB):
                tiles[pl.ds((b * EXT + 1) * 8 + 3 * t + c, ROWS, stride=8), :] = v[:, b * 128 : (b + 1) * 128]


def read_tiles(tiles, k):
    return jnp.concatenate([tiles[pl.ds((b * EXT + 1) * 8 + k, ROWS, stride=8), :] for b in range(NB)], axis=1)


def fill_halo(tiles, up, down):
    for b in range(NB):
        tiles[pl.ds(b * EXT * 8, 8), :] = up[:, b * 128 : (b + 1) * 128]
        tiles[pl.ds((b * EXT + EXT - 1) * 8, 8), :] = down[:, b * 128 : (b + 1) * 128]


def selectors():
    row = lax.broadcasted_iota(jnp.int32, (18, 768), 0)
    lane = lax.broadcasted_iota(jnp.int32, (18, 768), 1)
    return (lax.rem(row, 6) == lane // 128).astype(F32).astype(BF16)


def pieces(x):
    high = x.astype(BF16).astype(F32)
    rest = x - high
    middle = rest.astype(BF16).astype(F32)
    return [v[:6] for v in (high, middle, rest - middle)]


def flat(x):
    return jnp.concatenate([x[k : k + 1] for k in range(6)], axis=1)


def spread(left, right):
    return lax.dot_general(left.astype(BF16), right, (((0,), (0,)), ((), ())), preferred_element_type=F32)


def differences(on_lanes, on_sublanes, marks):
    left = jnp.concatenate([-v for v in pieces(on_sublanes)] + [jnp.ones((3, 128), F32)], axis=0)
    right = jnp.concatenate([marks] + [flat(v).astype(BF16) for v in pieces(on_lanes)], axis=0)
    return spread(left, right)


def block(x, j, k):
    return x[8 * j : 8 * j + 8, 128 * k : 128 * k + 128]


def stacked(rows):
    return jnp.concatenate([jnp.sum(v, axis=0, keepdims=True) for v in rows] + [jnp.zeros((2, 128), F32)], axis=0)


def pair_force(xa, xb, marks, scale):
    diff = differences(xa, xb, marks)
    rows = []
    for t in range(2):
        acc = [jnp.zeros((8, 128), F32) for _ in range(3)]
        for j in range(16):
            d = [block(diff, j, 3 * t + c) for c in range(3)]
            w = jnp.exp(-0.5 * (d[0] * d[0] + d[1] * d[1] + d[2] * d[2]))
            acc = [acc[c] + w * d[c] for c in range(3)]
        rows += acc
    return scale * stacked(rows)


def pair_adjoint(xa, xb, ga, marks, scale_a, scale_b):
    from_a = differences(xa, xb, marks)
    from_b = differences(xb, xa, marks)
    g_sub = spread(jnp.concatenate(pieces(ga), axis=0), marks)
    zero = jnp.zeros((8, 128), F32)
    rows_a, rows_b = [], []
    for t in range(2):
        g = [ga[3 * t + c : 3 * t + c + 1, :] for c in range(3)]
        weights, products = [], []
        sum_w = zero
        sum_a = [zero] * 3
        for j in range(16):
            d = [block(from_a, j, 3 * t + c) for c in range(3)]
            w = jnp.exp(-0.5 * (d[0] * d[0] + d[1] * d[1] + d[2] * d[2]))
            u = w * (g[0] * d[0] + g[1] * d[1] + g[2] * d[2])
            weights.append(w)
            products.append(u)
            sum_w = sum_w + w
            sum_a = [sum_a[c] + u * d[c] for c in range(3)]
        total = jnp.sum(sum_w, axis=0, keepdims=True)
        rows_a += [g[c] * total - jnp.sum(sum_a[c], axis=0, keepdims=True) for c in range(3)]
        w_back = jnp.transpose(jnp.concatenate(weights, axis=0))
        u_back = jnp.transpose(jnp.concatenate(products, axis=0))
        sum_b = [zero] * 3
        for j in range(16):
            w, u = w_back[8 * j : 8 * j + 8], u_back[8 * j : 8 * j + 8]
            sum_b = [sum_b[c] + (w * block(g_sub, j, 3 * t + c) + u * block(from_b, j, 3 * t + c)) for c in range(3)]
        rows_b += [jnp.sum(v, axis=0, keepdims=True) for v in sum_b]
    rest = [jnp.zeros((2, 128), F32)]
    return scale_a * jnp.concatenate(rows_a + rest, axis=0), -scale_b * jnp.concatenate(rows_b + rest, axis=0)


def pair_adjoint_far(xa, xb, ga, marks):
    from_b = differences(xb, xa, marks)
    g_sub = spread(jnp.concatenate(pieces(ga), axis=0), marks)
    rows = []
    for t in range(2):
        total = [jnp.zeros((8, 128), F32) for _ in range(3)]
        for j in range(16):
            total = pair_sum(total, [block(from_b, j, 3 * t + c) for c in range(3)], [block(g_sub, j, 3 * t + c) for c in range(3)])
        rows += total
    return -SCALE * stacked(rows)


def pair_sum(total, d, g):
    w = jnp.exp(-0.5 * (d[0] * d[0] + d[1] * d[1] + d[2] * d[2]))
    s = g[0] * d[0] + g[1] * d[1] + g[2] * d[2]
    return [v + w * (g[c] - s * d[c]) for c, v in enumerate(total)]


def edge_force(own, other, k):
    d = [o - x for o, x in zip(other, own)]
    coef = k * (1.0 - lax.rsqrt(d[0] * d[0] + d[1] * d[1] + d[2] * d[2] + TINY))
    return [coef * e for e in d]


def edge_adjoint(own, other, k, u):
    d = [o - x for o, x in zip(other, own)]
    y = lax.rsqrt(d[0] * d[0] + d[1] * d[1] + d[2] * d[2] + TINY)
    s = d[0] * u[0] + d[1] * u[1] + d[2] * u[2]
    one = 1.0 - y
    k1, k2 = k * one, k * (y * y * y) * s
    return [k1 * u[c] + k2 * d[c] for c in range(3)], one * s


def start_kernel(meta, state, stiff, send_x, send_p, kk):
    first = meta[0, META_C] == 0
    last = meta[0, META_Q] == 63
    column = lax.broadcasted_iota(jnp.int32, (ROWS, COLS), 1)
    kk[0] = jnp.where(column < COLS - 1, stiff[0], 0.0)
    kc = jnp.where(jnp.logical_and(row_is(ROWS - 1), last), 0.0, stiff[1])
    kk[1] = kc
    write_sends(first, [state[t, c] for t in range(2) for c in range(3)], kc, send_x, send_p)


def write_sends(first, values, kc, send_x, send_p):
    tops = jnp.concatenate([v[0:1] for v in values] + [kc[7:8], kc[7:8]], axis=0)
    lows = jnp.concatenate([v[7:8] for v in values] + [kc[7:8], kc[7:8]], axis=0)
    send_x[...] = jnp.where(first, tops, lows)
    send_p[...] = jnp.where(first, lows, tops)


def side_row(first, v, outer):
    return jnp.where(first, v[0:1], v[7:8]) if outer else jnp.where(first, v[7:8], v[0:1])


def forward_inner(step, meta, state, halo_p, kk, force, tiles, acc):
    first = meta[0, META_C] == 0
    row, base = lists(meta, step)
    fill_tiles(tiles, lambda t, c: state[t, c])
    fill_halo(tiles, halo_p[...], halo_p[...])
    acc[...] = jnp.zeros(acc.shape, F32)
    outer = jnp.where(first, 0, EXT - 1)

    count = meta[row, base + 2 * SLOTS]
    marks = selectors()

    def group(i, carry):
        results = []
        for q in range(GROUP):
            p = i * GROUP + q
            a = meta[row, base + p]
            b = meta[row, base + SLOTS + p]
            b_row = b // NB
            live = jnp.logical_and(p < count, b_row != outer)
            at = tile_start(a // NB + 1, lax.rem(a, NB))
            xa = tiles[pl.ds(at, 8), :]
            xb = tiles[pl.ds(tile_start(b_row, lax.rem(b, NB)), 8), :]
            results.append((at, pair_force(xa, xb, marks, jnp.where(live, SCALE, 0.0))))
        for at, value in results:
            acc[pl.ds(at, 8), :] += value
        return carry

    lax.fori_loop(0, (count + GROUP - 1) // GROUP, group, 0)
    kh, kc = kk[0], kk[1]
    k_up = jnp.where(row_is(0), 0.0, pltpu.roll(kc, 1, 0))
    k_side = jnp.where(first, kc[7:8], halo_p[6:7])
    side = jnp.where(first, ROWS - 1, 0)
    for t in range(2):
        x = [state[t, c] for c in range(3)]
        right = edge_force(x, [pltpu.roll(v, COLS - 1, 1) for v in x], kh)
        up = edge_force(x, [pltpu.roll(v, 1, 0) for v in x], k_up)
        edge = edge_force([side_row(first, v, False) for v in x], [halo_p[3 * t + c : 3 * t + c + 1] for c in range(3)], k_side)
        for c in range(3):
            total = right[c] - pltpu.roll(right[c], 1, 1) + up[c] - pltpu.roll(up[c], 7, 0)
            force[3 * t + c] = total + jnp.where(row_is(side), edge[c], 0.0) + read_tiles(acc, 3 * t + c)


def forward_outer(step, meta, state, halo_x, kk, force, state_out, send_x, send_p, tiles, acc, halo):
    first = meta[0, META_C] == 0
    row, base = lists(meta, step)
    count = meta[row, base + 2 * SLOTS]
    outer = jnp.where(first, 0, EXT - 1)
    hits = [jnp.logical_and(p < count, meta[row, base + SLOTS + p] // NB == outer) for p in range(SLOTS)]
    some = functools.reduce(jnp.logical_or, hits)

    @pl.when(some)
    def _():
        acc[...] = jnp.zeros(acc.shape, F32)
        fill_tiles(tiles, lambda t, c: state[t, c])
        for b in range(NB):
            halo[pl.ds(8 * b, 8), :] = halo_x[:, b * 128 : (b + 1) * 128]
        marks = selectors()

        def slot(p, carry):
            a = meta[row, base + p]
            b = meta[row, base + SLOTS + p]

            @pl.when(b // NB == outer)
            def _():
                at = tile_start(a // NB + 1, lax.rem(a, NB))
                xa = tiles[pl.ds(at, 8), :]
                xb = halo[pl.ds(pl.multiple_of(8 * lax.rem(b, NB), 8), 8), :]
                acc[pl.ds(at, 8), :] += pair_force(xa, xb, marks, SCALE)

            return carry

        lax.fori_loop(0, count, slot, 0)
        for k in range(6):
            force[k] = force[k] + read_tiles(acc, k)

    kc = kk[1]
    k_side = jnp.where(first, halo_x[6:7], kc[7:8])
    side = jnp.where(first, 0, ROWS - 1)
    values = []
    for t in range(2):
        x = [state[t, c] for c in range(3)]
        edge = edge_force([side_row(first, v, True) for v in x], [halo_x[3 * t + c : 3 * t + c + 1] for c in range(3)], k_side)
        for c in range(3):
            f = force[3 * t + c] + jnp.where(row_is(side), edge[c], 0.0)
            if c == 2:
                f = f - GRAV
            v = DAMP * (state[t, 3 + c] + H * f)
            new = x[c] + H * v
            state_out[t, c] = new
            state_out[t, 3 + c] = v
            values.append(new)
    write_sends(first, values, kc, send_x, send_p)


def joined(first, lam, got_x, got_p):
    up = jnp.where(first, got_x[...], got_p[...])
    down = jnp.where(first, got_p[...], got_x[...])
    result = []
    for t in range(2):
        for c in range(3):
            k = 3 * t + c
            result.append(lam[t, c] + jnp.where(row_is(0), up[k : k + 1], 0.0) + jnp.where(row_is(7), down[k : k + 1], 0.0))
    return result, down[6:7]


def backward_outer(step, opening, keep, meta, lam, *refs):
    refs = list(refs)
    got = None if opening else (refs.pop(0), refs.pop(0))
    state, halo_x, halo_p, kk, lam_out, send_x, send_p, kd = refs[:8]
    refs = refs[8:]
    full = refs.pop(0) if keep else None
    tiles, grads, acc_b = refs
    first = meta[0, META_C] == 0
    row, base = lists(meta, step)
    count = meta[row, base + 2 * SLOTS]
    if opening:
        xbar = [lam[t, c] for t in range(2) for c in range(3)]
        got_k = jnp.zeros((1, COLS), F32)
    else:
        xbar, got_k = joined(first, lam, *got)
    force = []
    for t in range(2):
        for c in range(3):
            vbar = lam[t, 3 + c]
            if keep:
                full[t, c] = xbar[3 * t + c]
                full[t, 3 + c] = vbar
            a = DAMP * (vbar + H * xbar[3 * t + c])
            lam_out[t, 3 + c] = a
            force.append(H * a)
    up = jnp.where(first, halo_x[...], halo_p[...])
    down = jnp.where(first, halo_p[...], halo_x[...])
    kc = kk[1]
    up_rows, down_rows = [], []
    up_k = jnp.zeros((1, COLS), F32)
    down_k = got_k
    for t in range(2):
        x = [state[t, c] for c in range(3)]
        g = force[3 * t : 3 * t + 3]
        eu, ku = edge_adjoint([v[0:1] for v in x], [up[3 * t + c : 3 * t + c + 1] for c in range(3)], up[6:7], [v[0:1] for v in g])
        ed, kw = edge_adjoint([v[7:8] for v in x], [down[3 * t + c : 3 * t + c + 1] for c in range(3)], kc[7:8], [v[7:8] for v in g])
        up_rows += eu
        down_rows += ed
        up_k = up_k + ku
        down_k = down_k + kw
        for c in range(3):
            lam_out[t, c] = xbar[3 * t + c] - jnp.where(row_is(0), eu[c], 0.0) - jnp.where(row_is(7), ed[c], 0.0)
    kd[...] = jnp.broadcast_to(down_k, (8, COLS))
    zero = jnp.zeros((1, COLS), F32)
    msg_up = jnp.concatenate(up_rows + [up_k, zero], axis=0)
    msg_down = jnp.concatenate(down_rows + [zero, zero], axis=0)
    send_x[...] = jnp.where(first, msg_up, msg_down)
    send_p[...] = jnp.where(first, msg_down, msg_up)

    def far(b):
        return jnp.logical_or(b < NB, b >= NB * (EXT - 1))

    hits = [jnp.logical_and(p < count, far(meta[row, base + SLOTS + p])) for p in range(SLOTS)]
    some = functools.reduce(jnp.logical_or, hits)

    @pl.when(some)
    def _():
        acc_b[...] = jnp.zeros(acc_b.shape, F32)
        fill_tiles(tiles, lambda t, c: state[t, c])
        fill_halo(tiles, up, down)
        fill_tiles(grads, lambda t, c: force[3 * t + c])
        marks = selectors()

        def slot(p, carry):
            a = meta[row, base + p]
            b = meta[row, base + SLOTS + p]

            @pl.when(far(b))
            def _():
                at = tile_start(a // NB + 1, lax.rem(a, NB))
                bt = tile_start(b // NB, lax.rem(b, NB))
                con_b = pair_adjoint_far(tiles[pl.ds(at, 8), :], tiles[pl.ds(bt, 8), :], grads[pl.ds(at, 8), :], marks)
                out = pl.multiple_of(8 * jnp.where(b < NB, b, b - NB * (EXT - 2)), 8)
                acc_b[pl.ds(out, 8), :] += con_b

            return carry

        lax.fori_loop(0, count, slot, 0)
        more_up = jnp.concatenate([acc_b[8 * b : 8 * b + 8, :] for b in range(NB)], axis=1)
        more_down = jnp.concatenate([acc_b[8 * (NB + b) : 8 * (NB + b) + 8, :] for b in range(NB)], axis=1)
        send_x[...] += jnp.where(first, more_up, more_down)
        send_p[...] += jnp.where(first, more_down, more_up)


def backward_inner(step, opening, meta, lam, state, halo_x, halo_p, kk, kd, *refs):
    refs = list(refs)
    old = None if opening else refs.pop(0)
    if step == COPY_STEP:
        source, target, sems, buffer = refs.pop(0), refs.pop(2), refs.pop(), refs.pop()
        fetch = pltpu.make_async_copy(source, buffer, sems.at[0])
        store = pltpu.make_async_copy(buffer, target, sems.at[1])
        fetch.start()
    lam_out, grad, tiles, grads, acc = refs
    row, base = lists(meta, step)
    last = meta[0, META_Q] == 63
    fill_tiles(tiles, lambda t, c: state[t, c])
    fill_tiles(grads, lambda t, c: H * lam[t, 3 + c])
    first = meta[0, META_C] == 0
    fill_halo(tiles, jnp.where(first, halo_x[...], halo_p[...]), jnp.where(first, halo_p[...], halo_x[...]))
    acc[...] = jnp.zeros(acc.shape, F32)
    count = meta[row, base + 2 * SLOTS]
    marks = selectors()

    def group(i, carry):
        results = []
        for q in range(GROUP_BACK):
            n = i * GROUP_BACK + q
            p = jnp.minimum(n, SLOTS - 1)
            a = meta[row, base + p]
            b = meta[row, base + SLOTS + p]
            live = n < count
            inside = jnp.logical_and(live, jnp.logical_and(b >= NB, b < NB * (EXT - 1)))
            at = tile_start(a // NB + 1, lax.rem(a, NB))
            bt = tile_start(b // NB, lax.rem(b, NB))
            scales = [jnp.where(on, SCALE, 0.0) for on in (live, inside)]
            results.append((at, bt, *pair_adjoint(tiles[pl.ds(at, 8), :], tiles[pl.ds(bt, 8), :], grads[pl.ds(at, 8), :], marks, *scales)))
        for at, bt, con_a, con_b in results:
            acc[pl.ds(at, 8), :] += con_a
            acc[pl.ds(bt, 8), :] += con_b
        return carry

    lax.fori_loop(0, (count + GROUP_BACK - 1) // GROUP_BACK, group, 0)
    if step == COPY_STEP:
        fetch.wait()
        store.start()
    kh, kc = kk[0], kk[1]
    k_up = jnp.where(row_is(0), 0.0, pltpu.roll(kc, 1, 0))
    grad_h = jnp.zeros((ROWS, COLS), F32)
    grad_v = jnp.zeros((ROWS, COLS), F32)
    for t in range(2):
        x = [state[t, c] for c in range(3)]
        g = [H * lam[t, 3 + c] for c in range(3)]
        right, rk = edge_adjoint(x, [pltpu.roll(v, COLS - 1, 1) for v in x], kh, [v - pltpu.roll(v, COLS - 1, 1) for v in g])
        up, uk = edge_adjoint(x, [pltpu.roll(v, 1, 0) for v in x], k_up, [v - pltpu.roll(v, 1, 0) for v in g])
        grad_h = grad_h + rk
        grad_v = grad_v + uk
        for c in range(3):
            total = pltpu.roll(right[c], 1, 1) - right[c] + pltpu.roll(up[c], 7, 0) - up[c]
            lam_out[t, c] = lam[t, c] + total + read_tiles(acc, 3 * t + c)
            lam_out[t, 3 + c] = lam[t, 3 + c]
    column = lax.broadcasted_iota(jnp.int32, (ROWS, COLS), 1)
    grad_h = jnp.where(column < COLS - 1, grad_h, 0.0)
    grad_v = jnp.where(row_is(7), jnp.where(last, 0.0, kd[0:1]), pltpu.roll(grad_v, 7, 0))
    if opening:
        grad[0] = grad_h
        grad[1] = grad_v
    else:
        grad[0] = old[0] + grad_h
        grad[1] = old[1] + grad_v
    if step == COPY_STEP:
        store.wait()


def end_kernel(meta, lam, got_x, got_p, old, out):
    first = meta[0, META_C] == 0
    last = meta[0, META_Q] == 63
    xbar, got_k = joined(first, lam, got_x, got_p)
    zero = jnp.zeros((2, COLS), F32)
    out[0] = old[0]
    out[1] = old[1] + jnp.where(row_is(7), jnp.where(last, 0.0, got_k), 0.0)
    out[2] = jnp.concatenate([v[0:1] for v in xbar] + [zero], axis=0)
    out[3] = jnp.concatenate([v[7:8] for v in xbar] + [zero], axis=0)


def output_kernel(sections, meta, swapped, *refs):
    shared, lams = refs[:sections], refs[sections : 2 * sections]
    adjoint, grad, buffer, total, sems = refs[2 * sections :]
    here = meta[0, META_S] == 0

    @pl.when(jnp.logical_not(here))
    def _():
        for s in range(sections):
            pltpu.make_async_copy(swapped.at[s], adjoint.at[s], sems.at[s]).start()

    @pl.when(here)
    def _():
        for s, lam in enumerate(lams):
            part = shared[-s % sections]
            for t in range(2):
                for c in range(3):
                    k = 3 * t + c
                    v = jnp.where(row_is(0), part[2, k : k + 1], lam[t, c])
                    buffer[s, t, c] = jnp.where(row_is(7), part[3, k : k + 1], v)
                    buffer[s, t, 3 + c] = lam[t, 3 + c]
            pltpu.make_async_copy(buffer.at[s], adjoint.at[s], sems.at[s]).start()

    for own in range(sections):

        @pl.when(meta[0, META_S] == own)
        def _(own=own):
            for k in range(2):
                value = shared[own % sections][k]
                for s in range(1, sections):
                    value = value + shared[(own - s) % sections][k]
                total[k] = value

    last = pltpu.make_async_copy(total, grad, sems.at[sections])
    last.start()
    for s in range(sections):
        pltpu.make_async_copy(buffer.at[s], adjoint.at[s], sems.at[s]).wait()
    last.wait()


STATE = jax.ShapeDtypeStruct((2, 6, ROWS, COLS), F32)
HALO = jax.ShapeDtypeStruct((8, COLS), F32)
CHUNKS = jax.ShapeDtypeStruct((4, 2, 6, ROWS, COLS), F32)
GRADS = jax.ShapeDtypeStruct((2, ROWS, COLS), F32)
TILES = pltpu.VMEM((EXT * NB * 8, 128), F32)
SMALL = pltpu.VMEM((NB * 8, 128), F32)


def call(body, outs, operands, scratch=(), flops=0, hbm=(), hbm_out=()):
    spaces = [pltpu.HBM if k in hbm else pltpu.VMEM if k else pltpu.SMEM for k in range(len(operands))]
    operands = [pltpu.with_memory_space_constraint(x, space) for x, space in zip(operands, spaces)]
    out_spaces = [pltpu.HBM if k in hbm_out else pltpu.VMEM for k in range(len(outs))]
    return pl.pallas_call(
        body,
        out_shape=[space(o.shape, o.dtype) for space, o in zip(out_spaces, outs)],
        in_specs=[pl.BlockSpec(memory_space=space) for space in spaces],
        out_specs=[pl.BlockSpec(memory_space=space) for space in out_spaces],
        scratch_shapes=list(scratch),
        cost_estimate=pl.CostEstimate(flops=flops, transcendentals=0, bytes_accessed=1 << 18) if flops else None,
    )(*operands)


def on_device(start_state, stiffness, contact_a, contact_b, pair_count, cotangent):
    section = lax.axis_index("section")
    space = lax.axis_index("space")
    sections = lax.axis_size("section")
    spaces = lax.axis_size("space")
    cross = [(i, i + 1) for i in range(1, spaces - 1, 2)]
    cross = cross + [(b, a) for a, b in cross]
    near = [(i, i ^ 1) for i in range(spaces)]
    steps = contact_a.shape[0] * sections

    facts = jnp.pad(jnp.stack([section, lax.rem(space, 2), space]).astype(jnp.int32), (META_S, 64 - META_S - 3))[None]
    own_list = facts + jnp.pad(
        jnp.concatenate([contact_a[:, 0], contact_b[:, 0], pair_count], axis=1), ((0, 0), (0, 31 - 2 * SLOTS))
    ).reshape(1, 64)
    others = []
    for k in range(1, sections):
        others.append(lax.ppermute(own_list, "section", [(i, (i + k) % sections) for i in range(sections)]))
    meta = jnp.concatenate([own_list] + others, axis=0)

    state = lax.dynamic_slice_in_dim(start_state, section * 2, 2, 0)
    lam = lax.dynamic_slice_in_dim(cotangent, section * 2, 2, 0)
    send_x, send_p, kk = call(start_kernel, [HALO, HALO, GRADS], [facts, state, stiffness])

    def exchange(send_x, send_p):
        got_x = lax.ppermute(send_x, "space", cross)
        got_p = lax.ppermute(send_p, "space", near)
        return got_x, got_p

    states, halos, exits = [], [], []
    for step in range(steps):
        halo_x, halo_p = exchange(send_x, send_p)
        (force,) = call(
            functools.partial(forward_inner, step),
            [jax.ShapeDtypeStruct((6, ROWS, COLS), F32)],
            [meta, state, halo_p, kk],
            [TILES, TILES],
            flops=4000000,
        )
        states.append(state)
        halos.append((halo_x, halo_p))
        state, send_x, send_p = call(
            functools.partial(forward_outer, step), [STATE, HALO, HALO], [meta, state, halo_x, kk, force], [TILES, TILES, SMALL]
        )
        if step % 2 == 1:
            exits.append(state)
    exit_state = lax.all_to_all(jnp.stack(exits), "section", 0, 0, tiled=True)

    grad = None
    got = ()
    fulls = []
    for step in reversed(range(steps)):
        opening = step == steps - 1
        keep = step % 2 == 1 and not opening
        lam, send_x, send_p, kd, *rest = call(
            functools.partial(backward_outer, step, opening, keep),
            [STATE, HALO, HALO, HALO] + [STATE] * keep,
            [meta, lam, *got, states[step], *halos[step], kk],
            [TILES, TILES, pltpu.VMEM((2 * NB * 8, 128), F32)],
        )
        fulls = rest + fulls
        got = exchange(send_x, send_p)
        copying = step == COPY_STEP
        operands = [meta, lam, states[step], *halos[step], kk, kd] + ([] if opening else [grad])
        lam, grad, *rest = call(
            functools.partial(backward_inner, step, opening),
            [STATE, GRADS] + [CHUNKS] * copying,
            operands + [exit_state] * copying,
            [TILES, TILES, TILES] + ([pltpu.VMEM(CHUNKS.shape, F32), pltpu.SemaphoreType.DMA((2,))] if copying else []),
            flops=8000000,
            hbm=(len(operands),),
            hbm_out=(2,),
        )
        if copying:
            (exit_state,) = rest
        if step == 1:
            swapped = lax.all_to_all(jnp.stack([fulls[0], *fulls]), "section", 0, 0, tiled=True)
    lams = [lam]
    for s in range(1, sections):
        lams.append(lax.ppermute(lam, "section", [(s, 0)]))
    (shared,) = call(end_kernel, [jax.ShapeDtypeStruct((4, ROWS, COLS), F32)], [meta, lam, *got, grad])
    parts = [shared] + [lax.ppermute(shared, "section", [(i, (i + k) % sections) for i in range(sections)]) for k in range(1, sections)]
    adjoint, stiffness_grad = call(
        functools.partial(output_kernel, sections),
        [CHUNKS, GRADS],
        [meta, swapped, *parts, *lams],
        [pltpu.VMEM((4, 2, 6, ROWS, COLS), F32), pltpu.VMEM((2, ROWS, COLS), F32), pltpu.SemaphoreType.DMA((5,))],
        hbm_out=(0, 1),
    )
    return (
        exit_state.reshape(1, 8, 6, ROWS, COLS),
        adjoint.reshape(1, 8, 6, ROWS, COLS),
        stiffness_grad,
    )


def solution(mesh):
    in_specs = (
        P(None, None, "space", None),
        P(None, "space", None),
        P("section", "space", None),
        P("section", "space", None),
        P("section", "space"),
        P(None, None, "space", None),
    )
    out_specs = (
        P("section", None, None, "space", None),
        P("section", None, None, "space", None),
        P(None, "space", None),
    )
    return jax.shard_map(on_device, mesh=mesh, in_specs=in_specs, out_specs=out_specs, check_vma=False)
```

```python
import functools

import jax
import jax.numpy as jnp
from jax import lax
from jax.experimental import pallas as pl
from jax.experimental.pallas import tpu as pltpu
from jax.sharding import PartitionSpec as P


H = 0.1
DAMP = 0.98
SCALE = 0.3
GRAV = 0.5
TINY = 1e-06
F32 = jnp.float32
BF16 = jnp.bfloat16
COPY_STEP = 3
GROUP = 2
GROUP_BACK = 2
SLOTS = 8
ROWS = 8
COLS = 512
NB = COLS // 128
EXT = ROWS + 2
META_S, META_C, META_Q = 24, 25, 26


def lists(meta, step):
    section = meta[0, META_S]
    row = lax.rem(section - step // 2 + 4, 4)
    base = 32 * (step % 2)
    return row, base


def tile_start(row, block):
    return pl.multiple_of((block * EXT + row) * 8, 8)


def row_is(r, n=COLS):
    return lax.broadcasted_iota(jnp.int32, (ROWS, n), 0) == r


def fill_tiles(tiles, value_of):
    for t in range(2):
        for c in range(3):
            v = value_of(t, c)
            for b in range(NB):
                tiles[pl.ds((b * EXT + 1) * 8 + 3 * t + c, ROWS, stride=8), :] = v[:, b * 128 : (b + 1) * 128]


def read_tiles(tiles, k):
    return jnp.concatenate([tiles[pl.ds((b * EXT + 1) * 8 + k, ROWS, stride=8), :] for b in range(NB)], axis=1)


def fill_halo(tiles, up, down):
    for b in range(NB):
        tiles[pl.ds(b * EXT * 8, 8), :] = up[:, b * 128 : (b + 1) * 128]
        tiles[pl.ds((b * EXT + EXT - 1) * 8, 8), :] = down[:, b * 128 : (b + 1) * 128]


def selectors():
    row = lax.broadcasted_iota(jnp.int32, (18, 768), 0)
    lane = lax.broadcasted_iota(jnp.int32, (18, 768), 1)
    return (lax.rem(row, 6) == lane // 128).astype(F32).astype(BF16)


def pieces(x):
    high = x.astype(BF16).astype(F32)
    rest = x - high
    middle = rest.astype(BF16).astype(F32)
    return [v[:6] for v in (high, middle, rest - middle)]


def flat(x):
    return jnp.concatenate([x[k : k + 1] for k in range(6)], axis=1)


def spread(left, right):
    return lax.dot_general(left.astype(BF16), right, (((0,), (0,)), ((), ())), preferred_element_type=F32)


def differences(on_lanes, on_sublanes, marks):
    left = jnp.concatenate([-v for v in pieces(on_sublanes)] + [jnp.ones((3, 128), F32)], axis=0)
    right = jnp.concatenate([marks] + [flat(v).astype(BF16) for v in pieces(on_lanes)], axis=0)
    return spread(left, right)


def block(x, j, k):
    return x[8 * j : 8 * j + 8, 128 * k : 128 * k + 128]


def stacked(rows):
    return jnp.concatenate([jnp.sum(v, axis=0, keepdims=True) for v in rows] + [jnp.zeros((2, 128), F32)], axis=0)


def pair_force(xa, xb, marks, scale):
    diff = differences(xa, xb, marks)
    rows = []
    for t in range(2):
        acc = [jnp.zeros((8, 128), F32) for _ in range(3)]
        for j in range(16):
            d = [block(diff, j, 3 * t + c) for c in range(3)]
            w = jnp.exp(-0.5 * (d[0] * d[0] + d[1] * d[1] + d[2] * d[2]))
            acc = [acc[c] + w * d[c] for c in range(3)]
        rows += acc
    return scale * stacked(rows)


def pair_adjoint(xa, xb, ga, marks, scale_a, scale_b):
    from_a = differences(xa, xb, marks)
    from_b = differences(xb, xa, marks)
    g_sub = spread(jnp.concatenate(pieces(ga), axis=0), marks)
    zero = jnp.zeros((8, 128), F32)
    rows_a, rows_b = [], []
    for t in range(2):
        g = [ga[3 * t + c : 3 * t + c + 1, :] for c in range(3)]
        weights, products = [], []
        sum_w = zero
        sum_a = [zero] * 3
        for j in range(16):
            d = [block(from_a, j, 3 * t + c) for c in range(3)]
            w = jnp.exp(-0.5 * (d[0] * d[0] + d[1] * d[1] + d[2] * d[2]))
            u = w * (g[0] * d[0] + g[1] * d[1] + g[2] * d[2])
            weights.append(w)
            products.append(u)
            sum_w = sum_w + w
            sum_a = [sum_a[c] + u * d[c] for c in range(3)]
        total = jnp.sum(sum_w, axis=0, keepdims=True)
        rows_a += [g[c] * total - jnp.sum(sum_a[c], axis=0, keepdims=True) for c in range(3)]
        w_back = jnp.transpose(jnp.concatenate(weights, axis=0))
        u_back = jnp.transpose(jnp.concatenate(products, axis=0))
        sum_b = [zero] * 3
        for j in range(16):
            w, u = w_back[8 * j : 8 * j + 8], u_back[8 * j : 8 * j + 8]
            sum_b = [sum_b[c] + (w * block(g_sub, j, 3 * t + c) + u * block(from_b, j, 3 * t + c)) for c in range(3)]
        rows_b += [jnp.sum(v, axis=0, keepdims=True) for v in sum_b]
    rest = [jnp.zeros((2, 128), F32)]
    return scale_a * jnp.concatenate(rows_a + rest, axis=0), -scale_b * jnp.concatenate(rows_b + rest, axis=0)


def pair_adjoint_far(xa, xb, ga, marks, scale):
    from_b = differences(xb, xa, marks)
    g_sub = spread(jnp.concatenate(pieces(ga), axis=0), marks)
    rows = []
    for t in range(2):
        total = [jnp.zeros((8, 128), F32) for _ in range(3)]
        for j in range(16):
            total = pair_sum(total, [block(from_b, j, 3 * t + c) for c in range(3)], [block(g_sub, j, 3 * t + c) for c in range(3)])
        rows += total
    return -scale * stacked(rows)


def pair_sum(total, d, g):
    w = jnp.exp(-0.5 * (d[0] * d[0] + d[1] * d[1] + d[2] * d[2]))
    s = g[0] * d[0] + g[1] * d[1] + g[2] * d[2]
    return [v + w * (g[c] - s * d[c]) for c, v in enumerate(total)]


def edge_force(own, other, k):
    d = [o - x for o, x in zip(other, own)]
    coef = k * (1.0 - lax.rsqrt(d[0] * d[0] + d[1] * d[1] + d[2] * d[2] + TINY))
    return [coef * e for e in d]


def edge_adjoint(own, other, k, u):
    d = [o - x for o, x in zip(other, own)]
    y = lax.rsqrt(d[0] * d[0] + d[1] * d[1] + d[2] * d[2] + TINY)
    s = d[0] * u[0] + d[1] * u[1] + d[2] * u[2]
    one = 1.0 - y
    k1, k2 = k * one, k * (y * y * y) * s
    return [k1 * u[c] + k2 * d[c] for c in range(3)], one * s


def start_kernel(meta, state, stiff, send_x, send_p, kk):
    first = meta[0, META_C] == 0
    last = meta[0, META_Q] == 63
    column = lax.broadcasted_iota(jnp.int32, (ROWS, COLS), 1)
    kk[0] = jnp.where(column < COLS - 1, stiff[0], 0.0)
    kc = jnp.where(jnp.logical_and(row_is(ROWS - 1), last), 0.0, stiff[1])
    kk[1] = kc
    write_sends(first, [state[t, c] for t in range(2) for c in range(3)], kc, send_x, send_p)


def write_sends(first, values, kc, send_x, send_p):
    tops = jnp.concatenate([v[0:1] for v in values] + [kc[7:8], kc[7:8]], axis=0)
    lows = jnp.concatenate([v[7:8] for v in values] + [kc[7:8], kc[7:8]], axis=0)
    send_x[...] = jnp.where(first, tops, lows)
    send_p[...] = jnp.where(first, lows, tops)


def side_row(first, v, outer):
    return jnp.where(first, v[0:1], v[7:8]) if outer else jnp.where(first, v[7:8], v[0:1])


def forward_inner(step, meta, state, halo_p, kk, force, tiles, acc):
    first = meta[0, META_C] == 0
    row, base = lists(meta, step)
    fill_tiles(tiles, lambda t, c: state[t, c])
    fill_halo(tiles, halo_p[...], halo_p[...])
    acc[...] = jnp.zeros(acc.shape, F32)
    outer = jnp.where(first, 0, EXT - 1)

    count = meta[row, base + 2 * SLOTS]
    marks = selectors()

    def group(i, carry):
        results = []
        for q in range(GROUP):
            p = i * GROUP + q
            a = meta[row, base + p]
            b = meta[row, base + SLOTS + p]
            b_row = b // NB
            live = jnp.logical_and(p < count, b_row != outer)
            at = tile_start(a // NB + 1, lax.rem(a, NB))
            xa = tiles[pl.ds(at, 8), :]
            xb = tiles[pl.ds(tile_start(b_row, lax.rem(b, NB)), 8), :]
            results.append((at, pair_force(xa, xb, marks, jnp.where(live, SCALE, 0.0))))
        for at, value in results:
            acc[pl.ds(at, 8), :] += value
        return carry

    lax.fori_loop(0, (count + GROUP - 1) // GROUP, group, 0)
    kh, kc = kk[0], kk[1]
    k_up = jnp.where(row_is(0), 0.0, pltpu.roll(kc, 1, 0))
    k_side = jnp.where(first, kc[7:8], halo_p[6:7])
    side = jnp.where(first, ROWS - 1, 0)
    for t in range(2):
        x = [state[t, c] for c in range(3)]
        right = edge_force(x, [pltpu.roll(v, COLS - 1, 1) for v in x], kh)
        up = edge_force(x, [pltpu.roll(v, 1, 0) for v in x], k_up)
        edge = edge_force([side_row(first, v, False) for v in x], [halo_p[3 * t + c : 3 * t + c + 1] for c in range(3)], k_side)
        for c in range(3):
            total = right[c] - pltpu.roll(right[c], 1, 1) + up[c] - pltpu.roll(up[c], 7, 0)
            force[3 * t + c] = total + jnp.where(row_is(side), edge[c], 0.0) + read_tiles(acc, 3 * t + c)


def forward_outer(step, meta, state, halo_x, kk, force, state_out, send_x, send_p, tiles, acc, halo):
    first = meta[0, META_C] == 0
    row, base = lists(meta, step)
    count = meta[row, base + 2 * SLOTS]
    outer = jnp.where(first, 0, EXT - 1)
    hits = [jnp.logical_and(p < count, meta[row, base + SLOTS + p] // NB == outer) for p in range(SLOTS)]
    some = functools.reduce(jnp.logical_or, hits)

    @pl.when(some)
    def _():
        acc[...] = jnp.zeros(acc.shape, F32)
        fill_tiles(tiles, lambda t, c: state[t, c])
        for b in range(NB):
            halo[pl.ds(8 * b, 8), :] = halo_x[:, b * 128 : (b + 1) * 128]
        marks = selectors()

        def slot(p, carry):
            a = meta[row, base + p]
            b = meta[row, base + SLOTS + p]

            @pl.when(b // NB == outer)
            def _():
                at = tile_start(a // NB + 1, lax.rem(a, NB))
                xa = tiles[pl.ds(at, 8), :]
                xb = halo[pl.ds(pl.multiple_of(8 * lax.rem(b, NB), 8), 8), :]
                acc[pl.ds(at, 8), :] += pair_force(xa, xb, marks, SCALE)

            return carry

        lax.fori_loop(0, count, slot, 0)
        for k in range(6):
            force[k] = force[k] + read_tiles(acc, k)

    kc = kk[1]
    k_side = jnp.where(first, halo_x[6:7], kc[7:8])
    side = jnp.where(first, 0, ROWS - 1)
    values = []
    for t in range(2):
        x = [state[t, c] for c in range(3)]
        edge = edge_force([side_row(first, v, True) for v in x], [halo_x[3 * t + c : 3 * t + c + 1] for c in range(3)], k_side)
        for c in range(3):
            f = force[3 * t + c] + jnp.where(row_is(side), edge[c], 0.0)
            if c == 2:
                f = f - GRAV
            v = DAMP * (state[t, 3 + c] + H * f)
            new = x[c] + H * v
            state_out[t, c] = new
            state_out[t, 3 + c] = v
            values.append(new)
    write_sends(first, values, kc, send_x, send_p)


def joined(first, lam, got_x, got_p):
    up = jnp.where(first, got_x[...], got_p[...])
    down = jnp.where(first, got_p[...], got_x[...])
    result = []
    for t in range(2):
        for c in range(3):
            k = 3 * t + c
            result.append(lam[t, c] + jnp.where(row_is(0), up[k : k + 1], 0.0) + jnp.where(row_is(7), down[k : k + 1], 0.0))
    return result, down[6:7]


def backward_outer(step, opening, keep, meta, lam, *refs):
    refs = list(refs)
    got = None if opening else (refs.pop(0), refs.pop(0))
    state, halo_x, halo_p, kk, lam_out, send_x, send_p, kd = refs[:8]
    refs = refs[8:]
    full = refs.pop(0) if keep else None
    tiles, grads, acc_b, packed = refs
    first = meta[0, META_C] == 0
    row, base = lists(meta, step)
    count = meta[row, base + 2 * SLOTS]
    if opening:
        xbar = [lam[t, c] for t in range(2) for c in range(3)]
        got_k = jnp.zeros((1, COLS), F32)
    else:
        xbar, got_k = joined(first, lam, *got)
    force = []
    for t in range(2):
        for c in range(3):
            vbar = lam[t, 3 + c]
            if keep:
                full[t, c] = xbar[3 * t + c]
                full[t, 3 + c] = vbar
            a = DAMP * (vbar + H * xbar[3 * t + c])
            lam_out[t, 3 + c] = a
            force.append(H * a)
    up = jnp.where(first, halo_x[...], halo_p[...])
    down = jnp.where(first, halo_p[...], halo_x[...])
    kc = kk[1]
    up_rows, down_rows = [], []
    up_k = jnp.zeros((1, COLS), F32)
    down_k = got_k
    for t in range(2):
        x = [state[t, c] for c in range(3)]
        g = force[3 * t : 3 * t + 3]
        eu, ku = edge_adjoint([v[0:1] for v in x], [up[3 * t + c : 3 * t + c + 1] for c in range(3)], up[6:7], [v[0:1] for v in g])
        ed, kw = edge_adjoint([v[7:8] for v in x], [down[3 * t + c : 3 * t + c + 1] for c in range(3)], kc[7:8], [v[7:8] for v in g])
        up_rows += eu
        down_rows += ed
        up_k = up_k + ku
        down_k = down_k + kw
        for c in range(3):
            lam_out[t, c] = xbar[3 * t + c] - jnp.where(row_is(0), eu[c], 0.0) - jnp.where(row_is(7), ed[c], 0.0)
    kd[...] = jnp.broadcast_to(down_k, (8, COLS))
    zero = jnp.zeros((1, COLS), F32)
    msg_up = jnp.concatenate(up_rows + [up_k, zero], axis=0)
    msg_down = jnp.concatenate(down_rows + [zero, zero], axis=0)
    send_x[...] = jnp.where(first, msg_up, msg_down)
    send_p[...] = jnp.where(first, msg_down, msg_up)

    def far(b):
        return jnp.logical_or(b < NB, b >= NB * (EXT - 1))

    found = jnp.int32(0)
    for p in range(SLOTS):
        packed[found] = p
        found = found + jnp.logical_and(p < count, far(meta[row, base + SLOTS + p])).astype(jnp.int32)

    @pl.when(found > 0)
    def _():
        acc_b[...] = jnp.zeros(acc_b.shape, F32)
        fill_tiles(tiles, lambda t, c: state[t, c])
        fill_halo(tiles, up, down)
        fill_tiles(grads, lambda t, c: force[3 * t + c])
        marks = selectors()

        def group(i, carry):
            results = []
            for q in range(2):
                n = 2 * i + q
                p = packed[jnp.minimum(n, found - 1)]
                a = meta[row, base + p]
                b = meta[row, base + SLOTS + p]
                at = tile_start(a // NB + 1, lax.rem(a, NB))
                bt = tile_start(b // NB, lax.rem(b, NB))
                out = pl.multiple_of(8 * jnp.where(b < NB, b, b - NB * (EXT - 2)), 8)
                scale = jnp.where(n < found, SCALE, 0.0)
                results.append((out, pair_adjoint_far(tiles[pl.ds(at, 8), :], tiles[pl.ds(bt, 8), :], grads[pl.ds(at, 8), :], marks, scale)))
            for out, value in results:
                acc_b[pl.ds(out, 8), :] += value
            return carry

        lax.fori_loop(0, (found + 1) // 2, group, 0)
        more_up = jnp.concatenate([acc_b[8 * b : 8 * b + 8, :] for b in range(NB)], axis=1)
        more_down = jnp.concatenate([acc_b[8 * (NB + b) : 8 * (NB + b) + 8, :] for b in range(NB)], axis=1)
        send_x[...] += jnp.where(first, more_up, more_down)
        send_p[...] += jnp.where(first, more_down, more_up)


def backward_inner(step, opening, meta, lam, state, halo_x, halo_p, kk, kd, *refs):
    refs = list(refs)
    old = None if opening else refs.pop(0)
    if step == COPY_STEP:
        source, target, sems, buffer = refs.pop(0), refs.pop(2), refs.pop(), refs.pop()
        fetch = pltpu.make_async_copy(source, buffer, sems.at[0])
        store = pltpu.make_async_copy(buffer, target, sems.at[1])
        fetch.start()
    lam_out, grad, tiles, grads, acc = refs
    row, base = lists(meta, step)
    last = meta[0, META_Q] == 63
    fill_tiles(tiles, lambda t, c: state[t, c])
    fill_tiles(grads, lambda t, c: H * lam[t, 3 + c])
    first = meta[0, META_C] == 0
    fill_halo(tiles, jnp.where(first, halo_x[...], halo_p[...]), jnp.where(first, halo_p[...], halo_x[...]))
    acc[...] = jnp.zeros(acc.shape, F32)
    count = meta[row, base + 2 * SLOTS]
    marks = selectors()

    def group(i, carry):
        results = []
        for q in range(GROUP_BACK):
            n = i * GROUP_BACK + q
            p = jnp.minimum(n, SLOTS - 1)
            a = meta[row, base + p]
            b = meta[row, base + SLOTS + p]
            live = n < count
            inside = jnp.logical_and(live, jnp.logical_and(b >= NB, b < NB * (EXT - 1)))
            at = tile_start(a // NB + 1, lax.rem(a, NB))
            bt = tile_start(b // NB, lax.rem(b, NB))
            scales = [jnp.where(on, SCALE, 0.0) for on in (live, inside)]
            results.append((at, bt, *pair_adjoint(tiles[pl.ds(at, 8), :], tiles[pl.ds(bt, 8), :], grads[pl.ds(at, 8), :], marks, *scales)))
        for at, bt, con_a, con_b in results:
            acc[pl.ds(at, 8), :] += con_a
            acc[pl.ds(bt, 8), :] += con_b
        return carry

    lax.fori_loop(0, (count + GROUP_BACK - 1) // GROUP_BACK, group, 0)
    if step == COPY_STEP:
        fetch.wait()
        store.start()
    kh, kc = kk[0], kk[1]
    k_up = jnp.where(row_is(0), 0.0, pltpu.roll(kc, 1, 0))
    grad_h = jnp.zeros((ROWS, COLS), F32)
    grad_v = jnp.zeros((ROWS, COLS), F32)
    for t in range(2):
        x = [state[t, c] for c in range(3)]
        g = [H * lam[t, 3 + c] for c in range(3)]
        right, rk = edge_adjoint(x, [pltpu.roll(v, COLS - 1, 1) for v in x], kh, [v - pltpu.roll(v, COLS - 1, 1) for v in g])
        up, uk = edge_adjoint(x, [pltpu.roll(v, 1, 0) for v in x], k_up, [v - pltpu.roll(v, 1, 0) for v in g])
        grad_h = grad_h + rk
        grad_v = grad_v + uk
        for c in range(3):
            total = pltpu.roll(right[c], 1, 1) - right[c] + pltpu.roll(up[c], 7, 0) - up[c]
            lam_out[t, c] = lam[t, c] + total + read_tiles(acc, 3 * t + c)
            lam_out[t, 3 + c] = lam[t, 3 + c]
    column = lax.broadcasted_iota(jnp.int32, (ROWS, COLS), 1)
    grad_h = jnp.where(column < COLS - 1, grad_h, 0.0)
    grad_v = jnp.where(row_is(7), jnp.where(last, 0.0, kd[0:1]), pltpu.roll(grad_v, 7, 0))
    if opening:
        grad[0] = grad_h
        grad[1] = grad_v
    else:
        grad[0] = old[0] + grad_h
        grad[1] = old[1] + grad_v
    if step == COPY_STEP:
        store.wait()


def end_kernel(meta, lam, got_x, got_p, old, out):
    first = meta[0, META_C] == 0
    last = meta[0, META_Q] == 63
    xbar, got_k = joined(first, lam, got_x, got_p)
    zero = jnp.zeros((2, COLS), F32)
    out[0] = old[0]
    out[1] = old[1] + jnp.where(row_is(7), jnp.where(last, 0.0, got_k), 0.0)
    out[2] = jnp.concatenate([v[0:1] for v in xbar] + [zero], axis=0)
    out[3] = jnp.concatenate([v[7:8] for v in xbar] + [zero], axis=0)


def output_kernel(sections, meta, swapped, *refs):
    shared, lams = refs[:sections], refs[sections : 2 * sections]
    adjoint, grad, buffer, total, sems = refs[2 * sections :]
    here = meta[0, META_S] == 0

    @pl.when(jnp.logical_not(here))
    def _():
        for s in range(sections):
            pltpu.make_async_copy(swapped.at[s], adjoint.at[s], sems.at[s]).start()

    @pl.when(here)
    def _():
        for s, lam in enumerate(lams):
            part = shared[-s % sections]
            for t in range(2):
                for c in range(3):
                    k = 3 * t + c
                    v = jnp.where(row_is(0), part[2, k : k + 1], lam[t, c])
                    buffer[s, t, c] = jnp.where(row_is(7), part[3, k : k + 1], v)
                    buffer[s, t, 3 + c] = lam[t, 3 + c]
            pltpu.make_async_copy(buffer.at[s], adjoint.at[s], sems.at[s]).start()

    for own in range(sections):

        @pl.when(meta[0, META_S] == own)
        def _(own=own):
            for k in range(2):
                value = shared[own % sections][k]
                for s in range(1, sections):
                    value = value + shared[(own - s) % sections][k]
                total[k] = value

    last = pltpu.make_async_copy(total, grad, sems.at[sections])
    last.start()
    for s in range(sections):
        pltpu.make_async_copy(buffer.at[s], adjoint.at[s], sems.at[s]).wait()
    last.wait()


STATE = jax.ShapeDtypeStruct((2, 6, ROWS, COLS), F32)
HALO = jax.ShapeDtypeStruct((8, COLS), F32)
CHUNKS = jax.ShapeDtypeStruct((4, 2, 6, ROWS, COLS), F32)
GRADS = jax.ShapeDtypeStruct((2, ROWS, COLS), F32)
TILES = pltpu.VMEM((EXT * NB * 8, 128), F32)
SMALL = pltpu.VMEM((NB * 8, 128), F32)


def call(body, outs, operands, scratch=(), flops=0, hbm=(), hbm_out=()):
    spaces = [pltpu.HBM if k in hbm else pltpu.VMEM if k else pltpu.SMEM for k in range(len(operands))]
    operands = [pltpu.with_memory_space_constraint(x, space) for x, space in zip(operands, spaces)]
    out_spaces = [pltpu.HBM if k in hbm_out else pltpu.VMEM for k in range(len(outs))]
    return pl.pallas_call(
        body,
        out_shape=[space(o.shape, o.dtype) for space, o in zip(out_spaces, outs)],
        in_specs=[pl.BlockSpec(memory_space=space) for space in spaces],
        out_specs=[pl.BlockSpec(memory_space=space) for space in out_spaces],
        scratch_shapes=list(scratch),
        cost_estimate=pl.CostEstimate(flops=flops, transcendentals=0, bytes_accessed=1 << 18) if flops else None,
    )(*operands)


def on_device(start_state, stiffness, contact_a, contact_b, pair_count, cotangent):
    section = lax.axis_index("section")
    space = lax.axis_index("space")
    sections = lax.axis_size("section")
    spaces = lax.axis_size("space")
    cross = [(i, i + 1) for i in range(1, spaces - 1, 2)]
    cross = cross + [(b, a) for a, b in cross]
    near = [(i, i ^ 1) for i in range(spaces)]
    steps = contact_a.shape[0] * sections

    facts = jnp.pad(jnp.stack([section, lax.rem(space, 2), space]).astype(jnp.int32), (META_S, 64 - META_S - 3))[None]
    own_list = facts + jnp.pad(
        jnp.concatenate([contact_a[:, 0], contact_b[:, 0], pair_count], axis=1), ((0, 0), (0, 31 - 2 * SLOTS))
    ).reshape(1, 64)
    others = []
    for k in range(1, sections):
        others.append(lax.ppermute(own_list, "section", [(i, (i + k) % sections) for i in range(sections)]))
    meta = jnp.concatenate([own_list] + others, axis=0)

    state = lax.dynamic_slice_in_dim(start_state, section * 2, 2, 0)
    lam = lax.dynamic_slice_in_dim(cotangent, section * 2, 2, 0)
    send_x, send_p, kk = call(start_kernel, [HALO, HALO, GRADS], [facts, state, stiffness])

    def exchange(send_x, send_p):
        got_x = lax.ppermute(send_x, "space", cross)
        got_p = lax.ppermute(send_p, "space", near)
        return got_x, got_p

    states, halos, exits = [], [], []
    for step in range(steps):
        halo_x, halo_p = exchange(send_x, send_p)
        (force,) = call(
            functools.partial(forward_inner, step),
            [jax.ShapeDtypeStruct((6, ROWS, COLS), F32)],
            [meta, state, halo_p, kk],
            [TILES, TILES],
            flops=4000000,
        )
        states.append(state)
        halos.append((halo_x, halo_p))
        state, send_x, send_p = call(
            functools.partial(forward_outer, step), [STATE, HALO, HALO], [meta, state, halo_x, kk, force], [TILES, TILES, SMALL]
        )
        if step % 2 == 1:
            exits.append(state)
    exit_state = lax.all_to_all(jnp.stack(exits), "section", 0, 0, tiled=True)

    grad = None
    got = ()
    fulls = []
    for step in reversed(range(steps)):
        opening = step == steps - 1
        keep = step % 2 == 1 and not opening
        lam, send_x, send_p, kd, *rest = call(
            functools.partial(backward_outer, step, opening, keep),
            [STATE, HALO, HALO, HALO] + [STATE] * keep,
            [meta, lam, *got, states[step], *halos[step], kk],
            [TILES, TILES, pltpu.VMEM((2 * NB * 8, 128), F32), pltpu.SMEM((SLOTS + 1,), jnp.int32)],
        )
        fulls = rest + fulls
        got = exchange(send_x, send_p)
        copying = step == COPY_STEP
        operands = [meta, lam, states[step], *halos[step], kk, kd] + ([] if opening else [grad])
        lam, grad, *rest = call(
            functools.partial(backward_inner, step, opening),
            [STATE, GRADS] + [CHUNKS] * copying,
            operands + [exit_state] * copying,
            [TILES, TILES, TILES] + ([pltpu.VMEM(CHUNKS.shape, F32), pltpu.SemaphoreType.DMA((2,))] if copying else []),
            flops=8000000,
            hbm=(len(operands),),
            hbm_out=(2,),
        )
        if copying:
            (exit_state,) = rest
        if step == 1:
            swapped = lax.all_to_all(jnp.stack([fulls[0], *fulls]), "section", 0, 0, tiled=True)
    lams = [lam]
    for s in range(1, sections):
        lams.append(lax.ppermute(lam, "section", [(s, 0)]))
    (shared,) = call(end_kernel, [jax.ShapeDtypeStruct((4, ROWS, COLS), F32)], [meta, lam, *got, grad])
    parts = [shared] + [lax.ppermute(shared, "section", [(i, (i + k) % sections) for i in range(sections)]) for k in range(1, sections)]
    adjoint, stiffness_grad = call(
        functools.partial(output_kernel, sections),
        [CHUNKS, GRADS],
        [meta, swapped, *parts, *lams],
        [pltpu.VMEM((4, 2, 6, ROWS, COLS), F32), pltpu.VMEM((2, ROWS, COLS), F32), pltpu.SemaphoreType.DMA((5,))],
        hbm_out=(0, 1),
    )
    return (
        exit_state.reshape(1, 8, 6, ROWS, COLS),
        adjoint.reshape(1, 8, 6, ROWS, COLS),
        stiffness_grad,
    )


def solution(mesh):
    in_specs = (
        P(None, None, "space", None),
        P(None, "space", None),
        P("section", "space", None),
        P("section", "space", None),
        P("section", "space"),
        P(None, None, "space", None),
    )
    out_specs = (
        P("section", None, None, "space", None),
        P("section", None, None, "space", None),
        P(None, "space", None),
    )
    return jax.shard_map(on_device, mesh=mesh, in_specs=in_specs, out_specs=out_specs, check_vma=False)
```
